32 devices in a mesh: data: 2 (over x), model: 4 (over z), beam: 4 (over y, core).
Axes of the slice: x: 2, y: 2, z: 4, core: 2. Of those that a mesh axis runs over, the one named last changes fastest.
Arguments:
- x_embed: bfloat16 [128, 1024], P(('data', 'beam')), parts along dimension 0
- parent: int32 [4, 32], P('data'), parts along dimension 0
- position: int32 [], replicated
- score: float32 [128], P(('data', 'beam')), parts along dimension 0
- k_cache: bfloat16 [4, 128, 256, 16, 64], P(None, ('data', 'beam'), None, 'model'), parts along dimension 1
- v_cache: bfloat16 [4, 128, 256, 16, 64], P(None, ('data', 'beam'), None, 'model'), parts along dimension 1
- gain_attn: bfloat16 [4, 1024], replicated
- w_query: bfloat16 [4, 1024, 1024], P(None, None, 'model')
- w_key: bfloat16 [4, 1024, 1024], P(None, None, 'model')
- w_value: bfloat16 [4, 1024, 1024], P(None, None, 'model')
- w_out: bfloat16 [4, 1024, 1024], P(None, 'model')
- gain_mlp: bfloat16 [4, 1024], replicated
- w_gate: bfloat16 [4, 1024, 4096], P(None, None, 'model')
- w_up: bfloat16 [4, 1024, 4096], P(None, None, 'model')
- w_down: bfloat16 [4, 4096, 1024], P(None, 'model')
- gain_final: bfloat16 [1024], replicated
- w_vocab: bfloat16 [1024, 32128], P(None, 'model')
Outputs:
- output 1: bfloat16 [4, 128, 256, 16, 64], P(None, ('data', 'beam'), None, 'model'), parts along dimension 1
- output 2: bfloat16 [4, 128, 256, 16, 64], P(None, ('data', 'beam'), None, 'model'), parts along dimension 1
- output 3: float32 [128, 32128], P(('data', 'beam'), 'model'), parts along dimension 0
There are 2 independent parts. The reference program is written for one: setup_inputs(seed, part) draws one part's arguments, and reference() takes and returns one part's arrays. A program takes and returns all parts, laid end to end along the dimension named above; an argument that names none is the same for every part.
All inputs are finite; a program needn't handle non-finite values.
Results may differ from the reference program's by a relative error of at most 0.00139351.
Values are sent between devices in bfloat16 or wider.
A program may use at most 1 GiB of HBM per device.

```python
import jax
import jax.numpy as jnp
from jax import lax

D_MODEL = 1024
N_HEADS = 16
KV_HEADS = 16
HEAD_DIM = 64
FF_DIM = 4096
VOCAB_SIZE = 32128
BATCH = 64
BEAM_WIDTH = 32
CACHE_LEN = 256
LAYERS = 4

SENTENCES = BATCH // BEAM_WIDTH
GROUP_SIZE = N_HEADS // KV_HEADS
NORM_EPS = 1e-6
ROPE_BASE = 10000.0


def rms_norm(residual, gain):
    inv_rms = lax.rsqrt(jnp.mean(residual * residual, axis=-1, keepdims=True) + NORM_EPS)
    return (residual * inv_rms * gain.astype(jnp.float32)).astype(jnp.bfloat16)


def rope_rotate(vectors, position):
    half_dim = HEAD_DIM // 2
    inv_freq = ROPE_BASE ** (-jnp.arange(half_dim, dtype=jnp.float32) / half_dim)
    angles = position.astype(jnp.float32) * inv_freq
    cos_part = jnp.cos(angles)
    sin_part = jnp.sin(angles)
    lower_half = vectors[..., :half_dim]
    upper_half = vectors[..., half_dim:]
    return jnp.concatenate([lower_half * cos_part - upper_half * sin_part, upper_half * cos_part + lower_half * sin_part], axis=-1)


def draw_parent(key):
    key_lead, key_coin, key_any = jax.random.split(key, 3)
    lead_beam = jax.random.randint(key_lead, (SENTENCES, 1), 0, BEAM_WIDTH)
    coin_flip = jax.random.randint(key_coin, (SENTENCES, BEAM_WIDTH), 0, 2)
    any_beam = jax.random.randint(key_any, (SENTENCES, BEAM_WIDTH), 0, BEAM_WIDTH)
    beam_offset = jnp.where(coin_flip == 0, lead_beam, any_beam)
    sent_start = jnp.arange(SENTENCES, dtype=jnp.int32)[:, None] * BEAM_WIDTH
    return (sent_start + beam_offset).astype(jnp.int32)


def make_weight(key, shape, scale):
    return (jax.random.normal(key, shape, jnp.float32) * scale).astype(jnp.bfloat16)


def make_gain(key, shape):
    return (1.0 + 0.4 * jax.random.normal(key, shape, jnp.float32)).astype(jnp.bfloat16)


def setup_inputs(seed: int = 0, part: int = 0) -> dict:
    own_keys = jax.random.split(jax.random.fold_in(jax.random.key(seed), part), 6)
    shared_keys = jax.random.split(jax.random.key(seed + 1), 12)
    cache_shape = (LAYERS, BATCH, CACHE_LEN, KV_HEADS, HEAD_DIM)
    q_cols = N_HEADS * HEAD_DIM
    kv_cols = KV_HEADS * HEAD_DIM
    v_mean = jax.random.normal(own_keys[4], (LAYERS, BATCH, 1, KV_HEADS, HEAD_DIM), jnp.float32)
    return {
        'x_embed': jax.random.normal(own_keys[0], (BATCH, D_MODEL), jnp.float32).astype(jnp.bfloat16),
        'parent': draw_parent(own_keys[1]),
        'position': jax.random.randint(shared_keys[0], (), CACHE_LEN // 2, CACHE_LEN).astype(jnp.int32),
        'score': -jax.random.uniform(own_keys[2], (BATCH,), jnp.float32, 0.0, 8.0),
        'k_cache': (2.5 * jax.random.normal(own_keys[3], cache_shape, jnp.float32)).astype(jnp.bfloat16),
        'v_cache': (v_mean + jax.random.normal(own_keys[5], cache_shape, jnp.float32)).astype(jnp.bfloat16),
        'gain_attn': make_gain(shared_keys[1], (LAYERS, D_MODEL)),
        'w_query': make_weight(shared_keys[2], (LAYERS, D_MODEL, q_cols), D_MODEL ** -0.5),
        'w_key': make_weight(shared_keys[3], (LAYERS, D_MODEL, kv_cols), 2.5 * D_MODEL ** -0.5),
        'w_value': make_weight(shared_keys[4], (LAYERS, D_MODEL, kv_cols), D_MODEL ** -0.5),
        'w_out': make_weight(shared_keys[5], (LAYERS, q_cols, D_MODEL), q_cols ** -0.5),
        'gain_mlp': make_gain(shared_keys[6], (LAYERS, D_MODEL)),
        'w_gate': make_weight(shared_keys[7], (LAYERS, D_MODEL, FF_DIM), D_MODEL ** -0.5),
        'w_up': make_weight(shared_keys[8], (LAYERS, D_MODEL, FF_DIM), D_MODEL ** -0.5),
        'w_down': make_weight(shared_keys[9], (LAYERS, FF_DIM, D_MODEL), FF_DIM ** -0.5),
        'gain_final': make_gain(shared_keys[10], (D_MODEL,)),
        'w_vocab': make_weight(shared_keys[11], (D_MODEL, VOCAB_SIZE), 2.0 * D_MODEL ** -0.5),
    }


def reference(x_embed, parent, position, score, k_cache, v_cache, gain_attn, w_query, w_key, w_value, w_out, gain_mlp, w_gate, w_up, w_down, gain_final, w_vocab):
    flat_parent = parent.reshape(BATCH)
    slot_mask = (jnp.arange(CACHE_LEN, dtype=position.dtype) <= position)[None, None, None, :]

    def layer_step(residual, params):
        k_layer, v_layer, g_attn, wq_layer, wk_layer, wv_layer, wo_layer, g_mlp, wg_layer, wu_layer, wd_layer = params
        k_sel = k_layer[flat_parent]
        v_sel = v_layer[flat_parent]
        normed = rms_norm(residual, g_attn)
        q_rot = rope_rotate(jnp.dot(normed, wq_layer, preferred_element_type=jnp.float32).reshape(BATCH, N_HEADS, HEAD_DIM), position).astype(jnp.bfloat16)
        k_new = rope_rotate(jnp.dot(normed, wk_layer, preferred_element_type=jnp.float32).reshape(BATCH, KV_HEADS, HEAD_DIM), position).astype(jnp.bfloat16)
        v_new = jnp.dot(normed, wv_layer, preferred_element_type=jnp.float32).astype(jnp.bfloat16).reshape(BATCH, KV_HEADS, HEAD_DIM)
        k_sel = lax.dynamic_update_slice_in_dim(k_sel, k_new[:, None].astype(k_sel.dtype), position, axis=1)
        v_sel = lax.dynamic_update_slice_in_dim(v_sel, v_new[:, None].astype(v_sel.dtype), position, axis=1)
        q_grouped = q_rot.reshape(BATCH, KV_HEADS, GROUP_SIZE, HEAD_DIM)
        logits = jnp.einsum('bkgd,bskd->bkgs', q_grouped.astype(jnp.float32), k_sel.astype(jnp.float32)) * HEAD_DIM ** -0.5
        logits = jnp.where(slot_mask, logits, -jnp.inf)
        attn_prob = jax.nn.softmax(logits, axis=-1).astype(jnp.bfloat16)
        attn_out = jnp.einsum('bkgs,bskd->bkgd', attn_prob.astype(jnp.float32), v_sel.astype(jnp.float32)).astype(jnp.bfloat16)
        residual = residual + jnp.dot(attn_out.reshape(BATCH, N_HEADS * HEAD_DIM), wo_layer, preferred_element_type=jnp.float32)
        normed = rms_norm(residual, g_mlp)
        gate_proj = jnp.dot(normed, wg_layer, preferred_element_type=jnp.float32)
        up_proj = jnp.dot(normed, wu_layer, preferred_element_type=jnp.float32)
        hidden = (jax.nn.silu(gate_proj) * up_proj).astype(jnp.bfloat16)
        residual = residual + jnp.dot(hidden, wd_layer, preferred_element_type=jnp.float32)
        return residual, (k_sel, v_sel)

    residual, (k_out, v_out) = lax.scan(layer_step, x_embed.astype(jnp.float32), (k_cache, v_cache, gain_attn, w_query, w_key, w_value, w_out, gain_mlp, w_gate, w_up, w_down))
    logits = jnp.dot(rms_norm(residual, gain_final), w_vocab, preferred_element_type=jnp.float32)
    candidates = score[flat_parent][:, None] + jax.nn.log_softmax(logits, axis=-1)
    return k_out, v_out, candidates
```

```python
import functools

import jax
import jax.numpy as jnp
from jax import lax
from jax.experimental import pallas as pl
from jax.experimental.pallas import tpu as pltpu
from jax.sharding import PartitionSpec as P

NORM_EPS = 1e-6
ROPE_BASE = 10000.0
MESH = pl.DeviceIdType.MESH
F32 = jnp.float32
BF16 = jnp.bfloat16


def rms(res, gain):
    inv = lax.rsqrt(jnp.mean(res * res, axis=-1, keepdims=True) + NORM_EPS)
    return (res * inv * gain.astype(F32)).astype(BF16)


def dot(a, b):
    return jnp.dot(a, b, preferred_element_type=F32)


def dot_t(a, b):
    return lax.dot_general(a, b, (((1,), (1,)), ((), ())), preferred_element_type=F32)


def decode_kernel(cfg, *refs):
    L, B, D, HD, S, KH, FF, V, NM, SPAN = cfg
    (rows_ref, pos_ref, x_ref, rowsv_ref, score_ref, cos_ref, sin_ref, ga_ref, gm_ref, gf_ref,
     kc, vc, wq, wk, wv, wo, wg, wu, wd, wt, ko, vo, cand_ref) = refs[:23]
    scratch = list(refs[23:])
    kb = scratch[:L]
    vb = scratch[L:2 * L]
    (wqb, wkb, wvb, wob, wgb, wub, wdb, kst, vst, ar, stat, scb, res, qs, lg, pr, osc, lgt,
     sem_c, sem_w, sem_t, sem_st, bsend, brecv, asend, arecv, ssend, srecv, csend, crecv) = scratch[2 * L:]
    C = KH * HD
    me = lax.axis_index("model")
    beam = lax.axis_index("beam")
    spos = lax.rem(beam, SPAN)
    partner = beam - spos + lax.rem(spos + 1, SPAN)
    own = pl.ds(spos * B, B)

    def cache_local(l):
        return (pltpu.make_async_copy(kc.at[l], kb[l].at[own], sem_c.at[2 * l]),
                pltpu.make_async_copy(vc.at[l], vb[l].at[own], sem_c.at[2 * l + 1]))

    def cache_push(l):
        return tuple(pltpu.make_async_remote_copy(src_ref=c.at[l], dst_ref=buf[l].at[own], send_sem=bsend.at[2 * l + i],
                                                  recv_sem=brecv.at[2 * l + i], device_id={"beam": partner}, device_id_type=MESH)
                     for i, (c, buf) in enumerate(((kc, kb), (vc, vb))))

    weights = ((wq, wqb), (wk, wkb), (wv, wvb), (wo, wob), (wg, wgb), (wu, wub), (wd, wdb))

    def weight(l, i):
        src, buf = weights[i]
        return pltpu.make_async_copy(src.at[l], buf.at[l % 2], sem_w.at[(l % 2) * 7 + i])

    chunks = (kb[0], vb[0], kb[1], vb[1])
    CW = S
    NCH = D // CW

    NT = lgt.shape[0]
    TN = lgt.shape[2]

    def vocab(c, n, rows=TN):
        start = n * TN if isinstance(n, int) else pl.multiple_of(n * TN, TN)
        return pltpu.make_async_copy(wt.at[pl.ds(start, rows), c * CW:(c + 1) * CW], chunks[c].at[n, pl.ds(0, rows)],
                                     sem_t.at[c * NT + n])

    def vocab_all(act):
        def body(n, carry):
            for c in range(NCH):
                act(vocab(c, n))
            return carry
        full = V // TN
        lax.fori_loop(0, full, body, 0)
        if full < NT:
            for c in range(NCH):
                act(vocab(c, full, V - full * TN))

    for i in range(3):
        weight(0, i).start()
    for c in cache_local(0):
        c.start()

    barrier = pltpu.get_barrier_semaphore()
    for k in range(1, NM):
        pl.semaphore_signal(barrier, inc=1, device_id={"model": lax.rem(me + k, NM)}, device_id_type=MESH)
    pl.semaphore_signal(barrier, inc=1, device_id={"beam": partner}, device_id_type=MESH)
    pl.semaphore_wait(barrier, NM)

    for c in cache_push(0):
        c.start()
    score_copy = pltpu.make_async_remote_copy(src_ref=score_ref, dst_ref=scb.at[0], send_sem=csend, recv_sem=crecv,
                                              device_id={"beam": partner}, device_id_type=MESH)
    score_copy.start()
    for i in range(3, 7):
        weight(0, i).start()
    for i in range(7):
        weight(1, i).start()

    def reduce_copies(step):
        slot = step * NM + me
        return [pltpu.make_async_remote_copy(src_ref=ar.at[slot], dst_ref=ar.at[slot], send_sem=asend.at[step * (NM - 1) + k - 1],
                                             recv_sem=arecv.at[step * (NM - 1) + k - 1],
                                             device_id={"model": lax.rem(me + k, NM)}, device_id_type=MESH)
                for k in range(1, NM)]

    def reduce_start(step, value):
        ar[step * NM + me] = value
        copies = reduce_copies(step)
        for c in copies:
            c.start()
        return copies

    def reduce_finish(step, copies):
        for c in copies:
            c.wait_recv()
        total = ar[step * NM]
        for k in range(1, NM):
            total = total + ar[step * NM + k]
        return total

    pos = pos_ref[0]
    cos = cos_ref[...]
    sin = sin_ref[...]
    low = lax.rem(lax.broadcasted_iota(jnp.int32, (B, C), 1), HD) < HD // 2

    def rope(x):
        other = jnp.where(low, -pltpu.roll(x, C - HD // 2, 1), pltpu.roll(x, HD // 2, 1))
        return x * cos + other * sin

    head_of_lane = lax.broadcasted_iota(jnp.int32, (8, C), 1) // HD
    head_mask = head_of_lane == lax.broadcasted_iota(jnp.int32, (8, C), 0)
    slot = lax.broadcasted_iota(jnp.int32, (C, S), 1)
    here = slot == pos
    res[...] = x_ref[...].astype(F32)
    sends = [score_copy]

    for l in range(L):
        ws = l % 2
        h = rms(res[...], ga_ref[l:l + 1, :])
        for i in range(3):
            weight(l, i).wait()
        q = rope(dot(h, wqb[ws])).astype(BF16).astype(F32)
        k = rope(dot(h, wkb[ws])).astype(BF16).astype(F32)
        v = dot(h, wvb[ws]).astype(BF16).astype(F32)
        qs[...] = q * (HD ** -0.5)
        pad = jnp.zeros((128 - B, C), F32)
        k_cols = jnp.concatenate([k, pad], axis=0).T
        v_cols = jnp.concatenate([v, pad], axis=0).T
        for c in cache_local(l):
            c.wait()
        pushes = cache_push(l)
        pushes[0].wait_recv()
        if l > 0:
            pltpu.make_async_copy(kst, ko.at[l - 1], sem_st.at[0]).wait()
        for b in range(B):
            kept = jnp.where(here, jnp.broadcast_to(k_cols[:, b:b + 1], (C, S)).astype(BF16), kb[l][rows_ref[b]])
            kst[b] = kept
            qb = jnp.where(head_mask, jnp.broadcast_to(qs[b:b + 1, :], (8, C)), 0.0).astype(BF16)
            lg[b * 8:(b + 1) * 8, :] = dot(qb, kept)
        pltpu.make_async_copy(kst, ko.at[l], sem_st.at[0]).start()
        logits = lg[...]
        logits = jnp.where(lax.broadcasted_iota(jnp.int32, logits.shape, 1) <= pos, logits, -jnp.inf)
        e = jnp.exp(logits - jnp.max(logits, axis=-1, keepdims=True))
        pr[...] = e / jnp.sum(e, axis=-1, keepdims=True)
        pushes[1].wait_recv()
        if l > 0:
            pltpu.make_async_copy(vst, vo.at[l - 1], sem_st.at[1]).wait()
        for b in range(B):
            kept = jnp.where(here, jnp.broadcast_to(v_cols[:, b:b + 1], (C, S)).astype(BF16), vb[l][rows_ref[b]])
            vst[b] = kept
            ob = dot_t(pr[b * 8:(b + 1) * 8, :].astype(BF16), kept)
            osc[b:b + 1, :] = jnp.sum(jnp.where(head_mask, ob, 0.0), axis=0, keepdims=True)
        pltpu.make_async_copy(vst, vo.at[l], sem_st.at[1]).start()
        weight(l, 3).wait()
        copies = reduce_start(2 * l, dot(osc[...].astype(BF16), wob[ws]))
        sends += copies
        if l + 1 < L:
            for c in cache_local(l + 1):
                c.start()
            for c in cache_push(l + 1):
                c.start()
            if l + 2 < L:
                for i in range(4):
                    weight(l + 2, i).start()
        sends += list(pushes)
        if l == 2:
            vocab_all(lambda c: c.start())
        r = res[...] + reduce_finish(2 * l, copies)
        h = rms(r, gm_ref[l:l + 1, :])
        weight(l, 4).wait()
        weight(l, 5).wait()
        gate = dot(h, wgb[ws])
        up = dot(h, wub[ws])
        g = (gate * jax.nn.sigmoid(gate) * up).astype(BF16)
        weight(l, 6).wait()
        copies = reduce_start(2 * l + 1, dot(g, wdb[ws]))
        sends += copies
        if l + 2 < L:
            for i in range(4, 7):
                weight(l + 2, i).start()
        res[...] = r + reduce_finish(2 * l + 1, copies)

    h = rms(res[...], gf_ref[...])
    vocab_all(lambda c: c.wait())

    def tile(n, carry):
        acc = dot_t(h[:, 0:CW], chunks[0][n])
        for c in range(1, NCH):
            acc = acc + dot_t(h[:, c * CW:(c + 1) * CW], chunks[c][n])
        acc = jnp.where(lax.broadcasted_iota(jnp.int32, (B, TN), 1) + n * TN < V, acc, -jnp.inf)
        lgt[n] = acc
        return jnp.maximum(carry, acc)

    peak = lax.fori_loop(0, NT, tile, jnp.full((B, TN), -jnp.inf, F32))
    m = jnp.max(peak, axis=-1, keepdims=True)

    def add_exp(n, carry):
        return carry + jnp.exp(lgt[n] - m)

    s = jnp.sum(lax.fori_loop(0, NT, add_exp, jnp.zeros((B, TN), F32)), axis=-1, keepdims=True)
    stat[me, 0] = jnp.broadcast_to(m, (B, 128))
    stat[me, 1] = jnp.broadcast_to(s, (B, 128))
    copies = [pltpu.make_async_remote_copy(src_ref=stat.at[me], dst_ref=stat.at[me], send_sem=ssend.at[k - 1], recv_sem=srecv.at[k - 1],
                                           device_id={"model": lax.rem(me + k, NM)}, device_id_type=MESH) for k in range(1, NM)]
    for c in copies:
        c.start()
    sends += copies
    score_copy.wait_recv()
    mine = score_ref[0:1, :]
    theirs = scb[0, 0:1, :]
    lane = lax.broadcasted_iota(jnp.int32, (B, 128), 1)
    want = rowsv_ref[...]
    first = jnp.where(spos == 0, mine, theirs)
    second = jnp.where(spos == 0, theirs, mine)
    parent_score = jnp.sum(jnp.where(lane == want, first, 0.0) + jnp.where(lane == want - B, second, 0.0), axis=-1, keepdims=True)
    for c in copies:
        c.wait_recv()
    gm = stat[0, 0]
    for k in range(1, NM):
        gm = jnp.maximum(gm, stat[k, 0])
    gs = stat[0, 1] * jnp.exp(stat[0, 0] - gm)
    for k in range(1, NM):
        gs = gs + stat[k, 1] * jnp.exp(stat[k, 0] - gm)
    gm = gm[:, 0:1]
    log_s = jnp.log(gs)[:, 0:1]
    for n in range(NT):
        hi = min((n + 1) * TN, V)
        cand_ref[:, n * TN:hi] = parent_score + ((lgt[n] - gm) - log_s)[:, :hi - n * TN]
    pltpu.make_async_copy(kst, ko.at[L - 1], sem_st.at[0]).wait()
    pltpu.make_async_copy(vst, vo.at[L - 1], sem_st.at[1]).wait()
    for c in sends:
        c.wait_send()


def solution(mesh):
    data_beam = ('data', 'beam')
    cache_spec = P(None, data_beam, None, 'model', None)
    col_spec = P(None, None, 'model')
    row_spec = P(None, 'model', None)
    in_specs = (P(data_beam, None), P('data', None), P(), P(data_beam), cache_spec, cache_spec,
                P(), col_spec, col_spec, col_spec, row_spec, P(), col_spec, col_spec, row_spec, P(), P(None, 'model'))
    out_specs = (cache_spec, cache_spec, P(data_beam, 'model'))
    n_model = mesh.shape['model']

    def local_step(x_embed, parent, position, score, k_cache, v_cache, gain_attn, w_query, w_key, w_value, w_out, gain_mlp,
                   w_gate, w_up, w_down, gain_final, w_vocab):
        L, B, S, KH, HD = k_cache.shape
        D = x_embed.shape[1]
        C = KH * HD
        FF = w_gate.shape[2]
        V = w_vocab.shape[1]
        span = parent.shape[1] // B
        my_index = lax.axis_index('beam')
        base = (my_index // span) * span * B
        rows = lax.dynamic_slice(parent.reshape(-1), (my_index * B,), (B,)) - base
        half = HD // 2
        inv_freq = ROPE_BASE ** (-jnp.arange(half, dtype=F32) / half)
        angles = position.astype(F32) * inv_freq
        cos = jnp.tile(jnp.cos(angles), 2 * KH)[None]
        sin = jnp.tile(jnp.sin(angles), 2 * KH)[None]
        flat = lambda c: jnp.transpose(c, (0, 1, 3, 4, 2)).reshape(L, B, C, S)
        score_pad = jnp.broadcast_to(jnp.pad(score, (0, 128 - B))[None], (8, 128))
        cfg = (L, B, D, HD, S, KH, FF, V, n_model, span)
        any_spec = pl.BlockSpec(memory_space=pl.ANY)
        vm = pl.BlockSpec(memory_space=pltpu.VMEM)
        sm = pl.BlockSpec(memory_space=pltpu.SMEM)
        steps = 2 * L
        TN = C
        NT = -(-V // TN)
        dma = pltpu.SemaphoreType.DMA
        scratch = ([pltpu.VMEM((span * B, C, S), BF16) for _ in range(2 * L)]
                   + [pltpu.VMEM((2, D, C), BF16)] * 3 + [pltpu.VMEM((2, C, D), BF16)]
                   + [pltpu.VMEM((2, D, FF), BF16)] * 2 + [pltpu.VMEM((2, FF, D), BF16)]
                   + [pltpu.VMEM((B, C, S), BF16)] * 2
                   + [pltpu.VMEM((steps * n_model, B, D), F32), pltpu.VMEM((n_model, 2, B, 128), F32), pltpu.VMEM((1, 8, 128), F32),
                      pltpu.VMEM((B, D), F32), pltpu.VMEM((B, C), F32), pltpu.VMEM((B * 8, S), F32), pltpu.VMEM((B * 8, S), F32),
                      pltpu.VMEM((B, C), F32), pltpu.VMEM((NT, B, TN), F32),
                      dma((2 * L,)), dma((14,)), dma((D // S * NT,)), dma((2,)), dma((2 * L,)), dma((2 * L,)),
                      dma((steps * (n_model - 1),)), dma((steps * (n_model - 1),)), dma((n_model - 1,)), dma((n_model - 1,)),
                      dma, dma])
        k_out, v_out, cand = pl.pallas_call(
            functools.partial(decode_kernel, cfg),
            out_shape=(jax.ShapeDtypeStruct((L, B, C, S), BF16), jax.ShapeDtypeStruct((L, B, C, S), BF16),
                       jax.ShapeDtypeStruct((B, V), F32)),
            in_specs=[sm, sm, vm, vm, vm, vm, vm, vm, vm, vm] + [any_spec] * 10,
            out_specs=(any_spec, any_spec, vm),
            scratch_shapes=scratch,
            compiler_params=pltpu.CompilerParams(collective_id=0, has_side_effects=True, vmem_limit_bytes=64 * 1024 * 1024 - 65536),
            name="decode_step",
        )(rows, position.reshape(1), x_embed, jnp.broadcast_to(rows[:, None], (B, 128)), score_pad, cos, sin, gain_attn, gain_mlp,
          gain_final[None], flat(k_cache), flat(v_cache), w_query, w_key, w_value, w_out, w_gate, w_up, w_down, w_vocab.T)
        back = lambda c: jnp.transpose(c.reshape(L, B, KH, HD, S), (0, 1, 4, 2, 3))
        return back(k_out), back(v_out), cand

    return jax.shard_map(local_step, mesh=mesh, in_specs=in_specs, out_specs=out_specs, check_vma=False)
```

```python
import functools

import jax
import jax.numpy as jnp
import numpy as np
from jax import lax
from jax.experimental import pallas as pl
from jax.experimental.pallas import tpu as pltpu
from jax.sharding import PartitionSpec as P

NORM_EPS = 1e-6
ROPE_BASE = 10000.0
MESH = pl.DeviceIdType.MESH
F32 = jnp.float32
BF16 = jnp.bfloat16
LANES = 128
SUB = 8


def rms(res, gain):
    inv = lax.rsqrt(jnp.mean(res * res, axis=-1, keepdims=True) + NORM_EPS)
    return (res * inv * gain.astype(F32)).astype(BF16)


def dot(a, b):
    return jnp.dot(a, b, preferred_element_type=F32)


def dot_t(a, b):
    return lax.dot_general(a, b, (((1,), (1,)), ((), ())), preferred_element_type=F32)


def decode_kernel(cfg, *refs):
    L, B, D, HD, S, KH, FF, V, NM, SPAN = cfg
    (parent_ref, pos_ref, x_ref, score_ref, freq_ref, ga_ref, gm_ref, gf_ref,
     kc, vc, wq, wk, wv, wo, wg, wu, wd, wt, kst, vst, cand_ref,
     kb0, kb1, vb0, vb1, wqb, wkb, wvb, wob, wgb, wub, wdb, ar, stat, scb, res, qs, lg, pr, osc, lgt,
     sem_c, sem_w, sem_t, free, bsend, brecv, asend, arecv, ssend, srecv, csend, crecv) = refs
    kb = (kb0, kb1)
    vb = (vb0, vb1)
    C = KH * HD
    me = lax.axis_index("model")
    beam = lax.axis_index("beam")
    spos = lax.rem(beam, SPAN)
    sent = lax.div(beam, SPAN)
    partner = beam - spos + lax.rem(spos + 1, SPAN)
    own = pl.ds(spos * B, B)

    def cache_local(l):
        return (pltpu.make_async_copy(kc.at[l], kb[l % 2].at[own], sem_c.at[2 * l]),
                pltpu.make_async_copy(vc.at[l], vb[l % 2].at[own], sem_c.at[2 * l + 1]))

    def cache_push(l):
        return tuple(pltpu.make_async_remote_copy(src_ref=c.at[l], dst_ref=buf[l % 2].at[own], send_sem=bsend.at[2 * l + i],
                                                  recv_sem=brecv.at[2 * l + i], device_id={"beam": partner}, device_id_type=MESH)
                     for i, (c, buf) in enumerate(((kc, kb), (vc, vb))))

    weights = ((wq, wqb), (wk, wkb), (wv, wvb), (wo, wob), (wg, wgb), (wu, wub), (wd, wdb))

    def weight(l, i):
        src, buf = weights[i]
        return pltpu.make_async_copy(src.at[l], buf.at[l % 2], sem_w.at[(l % 2) * 7 + i])

    chunks = (kb0, vb0, kb1, vb1)
    NCH = D // S
    NT = lgt.shape[0]
    TN = lgt.shape[2]

    def vocab(c, n, rows=TN):
        start = n * TN if isinstance(n, int) else pl.multiple_of(n * TN, TN)
        return pltpu.make_async_copy(wt.at[pl.ds(start, rows), c * S:(c + 1) * S], chunks[c].at[n, pl.ds(0, rows)],
                                     sem_t.at[c * NT + n])

    def vocab_all(which, act):
        def body(n, carry):
            for c in which:
                act(vocab(c, n))
            return carry
        full = V // TN
        lax.fori_loop(0, full, body, 0)
        if full < NT:
            for c in which:
                act(vocab(c, full, V - full * TN))

    for i in range(3):
        weight(0, i).start()
    for c in cache_local(0):
        c.start()

    barrier = pltpu.get_barrier_semaphore()
    for k in range(1, NM):
        pl.semaphore_signal(barrier, inc=1, device_id={"model": lax.rem(me + k, NM)}, device_id_type=MESH)
    pl.semaphore_signal(barrier, inc=1, device_id={"beam": partner}, device_id_type=MESH)

    scb[0] = jnp.zeros((SUB, LANES), F32)
    scb[0, 0:1, 0:B] = score_ref[...]
    pos = pos_ref[0]
    angle = pos.astype(F32) * freq_ref[...]
    cos = jnp.cos(angle)
    sin = jnp.sin(angle)
    low = lax.rem(lax.broadcasted_iota(jnp.int32, (B, C), 1), HD) < HD // 2
    rows = [lax.rem(parent_ref[sent, spos * B + b], SPAN * B) for b in range(B)]

    pl.semaphore_wait(barrier, NM)

    for c in cache_push(0):
        c.start()
    score_copy = pltpu.make_async_remote_copy(src_ref=scb.at[0], dst_ref=scb.at[1], send_sem=csend, recv_sem=crecv,
                                              device_id={"beam": partner}, device_id_type=MESH)
    score_copy.start()
    for i in range(3, 7):
        weight(0, i).start()
    for i in range(7):
        weight(1, i).start()

    def reduce_copies(step):
        slot = step * NM + me
        return [pltpu.make_async_remote_copy(src_ref=ar.at[slot], dst_ref=ar.at[slot], send_sem=asend.at[step * (NM - 1) + k - 1],
                                             recv_sem=arecv.at[step * (NM - 1) + k - 1],
                                             device_id={"model": lax.rem(me + k, NM)}, device_id_type=MESH)
                for k in range(1, NM)]

    def reduce_start(step, value):
        ar[step * NM + me] = value
        copies = reduce_copies(step)
        for c in copies:
            c.start()
        return copies

    def reduce_finish(step, copies):
        for c in copies:
            c.wait_recv()
        total = ar[step * NM]
        for k in range(1, NM):
            total = total + ar[step * NM + k]
        return total

    def rope(x):
        other = jnp.where(low, -pltpu.roll(x, C - HD // 2, 1), pltpu.roll(x, HD // 2, 1))
        return x * cos + other * sin

    head_of_lane = lax.broadcasted_iota(jnp.int32, (SUB, C), 1) // HD
    head_mask = head_of_lane == lax.broadcasted_iota(jnp.int32, (SUB, C), 0)
    here = lax.broadcasted_iota(jnp.int32, (C, S), 1) == pos
    res[...] = x_ref[...].astype(F32)
    sends = [score_copy]

    for l in range(L):
        ws = l % 2
        h = rms(res[...], ga_ref[l:l + 1, :])
        for i in range(3):
            weight(l, i).wait()
        q = rope(dot(h, wqb[ws])).astype(BF16).astype(F32)
        k = rope(dot(h, wkb[ws])).astype(BF16).astype(F32)
        v = dot(h, wvb[ws]).astype(BF16).astype(F32)
        qs[...] = q * (HD ** -0.5)
        pad = jnp.zeros((LANES - B, C), F32)
        k_cols = jnp.concatenate([k, pad], axis=0).T
        v_cols = jnp.concatenate([v, pad], axis=0).T
        for c in cache_local(l):
            c.wait()
        pushes = cache_push(l)
        sends += list(pushes)
        pushes[0].wait_recv()
        for b in range(B):
            kept = jnp.where(here, jnp.broadcast_to(k_cols[:, b:b + 1], (C, S)).astype(BF16), kb[ws][rows[b]])
            kst[l, b] = kept
            qb = jnp.where(head_mask, jnp.broadcast_to(qs[b:b + 1, :], (SUB, C)), 0.0).astype(BF16)
            lg[b * SUB:(b + 1) * SUB, :] = dot(qb, kept)
        logits = lg[...]
        logits = jnp.where(lax.broadcasted_iota(jnp.int32, logits.shape, 1) <= pos, logits, -jnp.inf)
        e = jnp.exp(logits - jnp.max(logits, axis=-1, keepdims=True))
        pr[...] = e / jnp.sum(e, axis=-1, keepdims=True)
        pushes[1].wait_recv()
        for b in range(B):
            kept = jnp.where(here, jnp.broadcast_to(v_cols[:, b:b + 1], (C, S)).astype(BF16), vb[ws][rows[b]])
            vst[l, b] = kept
            ob = dot_t(pr[b * SUB:(b + 1) * SUB, :].astype(BF16), kept)
            osc[b:b + 1, :] = jnp.sum(jnp.where(head_mask, ob, 0.0), axis=0, keepdims=True)
        if l + 2 < L:
            pl.semaphore_signal(free, inc=1, device_id={"beam": partner}, device_id_type=MESH)
        weight(l, 3).wait()
        copies = reduce_start(2 * l, dot(osc[...].astype(BF16), wob[ws]))
        sends += copies
        if l + 1 < L:
            for c in cache_local(l + 1):
                c.start()
            if l + 1 >= 2:
                pl.semaphore_wait(free, 1)
            for c in cache_push(l + 1):
                c.start()
            if l + 2 < L:
                for i in range(4):
                    weight(l + 2, i).start()
        if l == L - 1:
            vocab_all(range(NCH), lambda c: c.start())
        r = res[...] + reduce_finish(2 * l, copies)
        h = rms(r, gm_ref[l:l + 1, :])
        weight(l, 4).wait()
        weight(l, 5).wait()
        gate = dot(h, wgb[ws])
        up = dot(h, wub[ws])
        g = (gate * jax.nn.sigmoid(gate) * up).astype(BF16)
        weight(l, 6).wait()
        copies = reduce_start(2 * l + 1, dot(g, wdb[ws]))
        sends += copies
        if l + 2 < L:
            for i in range(4, 7):
                weight(l + 2, i).start()
        res[...] = r + reduce_finish(2 * l + 1, copies)

    gf = gf_ref[...].astype(F32)
    h = rms(res[...], jnp.concatenate([gf[i:i + 1, :] for i in range(D // LANES)], axis=1))
    vocab_all(range(NCH), lambda c: c.wait())

    def tile(n, carry):
        acc = dot_t(h[:, 0:S], chunks[0][n])
        for c in range(1, NCH):
            acc = acc + dot_t(h[:, c * S:(c + 1) * S], chunks[c][n])
        acc = jnp.where(lax.broadcasted_iota(jnp.int32, (B, TN), 1) + n * TN < V, acc, -jnp.inf)
        lgt[n] = acc
        return jnp.maximum(carry, acc)

    peak = lax.fori_loop(0, NT, tile, jnp.full((B, TN), -jnp.inf, F32))
    m = jnp.max(peak, axis=-1, keepdims=True)

    def add_exp(n, carry):
        return carry + jnp.exp(lgt[n] - m)

    s = jnp.sum(lax.fori_loop(0, NT, add_exp, jnp.zeros((B, TN), F32)), axis=-1, keepdims=True)
    stat[me, 0] = jnp.broadcast_to(m, (B, LANES))
    stat[me, 1] = jnp.broadcast_to(s, (B, LANES))
    copies = [pltpu.make_async_remote_copy(src_ref=stat.at[me], dst_ref=stat.at[me], send_sem=ssend.at[k - 1], recv_sem=srecv.at[k - 1],
                                           device_id={"model": lax.rem(me + k, NM)}, device_id_type=MESH) for k in range(1, NM)]
    for c in copies:
        c.start()
    sends += copies
    score_copy.wait_recv()
    sub = lax.broadcasted_iota(jnp.int32, (B, LANES), 0)
    want = jnp.zeros((B, LANES), jnp.int32)
    for b in range(B):
        want = jnp.where(sub == b, rows[b], want)
    lane = lax.broadcasted_iota(jnp.int32, (B, LANES), 1)
    mine = jnp.where(lane + spos * B == want, scb[0, 0:1, :], 0.0)
    theirs = jnp.where(lane + (SPAN - 1 - spos) * B == want, scb[1, 0:1, :], 0.0)
    parent_score = jnp.sum(jnp.where(lane < B, mine + theirs, 0.0), axis=-1, keepdims=True)
    for c in copies:
        c.wait_recv()
    gm = stat[0, 0]
    for k in range(1, NM):
        gm = jnp.maximum(gm, stat[k, 0])
    gs = stat[0, 1] * jnp.exp(stat[0, 0] - gm)
    for k in range(1, NM):
        gs = gs + stat[k, 1] * jnp.exp(stat[k, 0] - gm)
    gm = gm[:, 0:1]
    log_s = jnp.log(gs)[:, 0:1]
    for n in range(NT):
        hi = min((n + 1) * TN, V)
        cand_ref[:, n * TN:hi] = parent_score + ((lgt[n] - gm) - log_s)[:, :hi - n * TN]
    for c in sends:
        c.wait_send()


def write_kernel(*refs):
    n = (len(refs) - 1) // 2
    sem = refs[-1]
    copies = []
    for i in range(n):
        src, dst = refs[i], refs[n + i]
        if len(src.shape) > 2:
            copies += [(src.at[j], dst.at[j]) for j in range(src.shape[0])]
        else:
            copies.append((src, dst))
    copies = [pltpu.make_async_copy(a, b, sem.at[j]) for j, (a, b) in enumerate(copies)]
    for c in copies:
        c.start()
    for c in copies:
        c.wait()


def solution(mesh):
    data_beam = ('data', 'beam')
    cache_spec = P(None, data_beam, None, 'model', None)
    col_spec = P(None, None, 'model')
    row_spec = P(None, 'model', None)
    in_specs = (P(data_beam, None), P('data', None), P(), P(data_beam), cache_spec, cache_spec,
                P(), col_spec, col_spec, col_spec, row_spec, P(), col_spec, col_spec, row_spec, P(), P(None, 'model'))
    out_specs = (cache_spec, cache_spec, P(data_beam, 'model'))
    n_model = mesh.shape['model']

    def local_step(x_embed, parent, position, score, k_cache, v_cache, gain_attn, w_query, w_key, w_value, w_out, gain_mlp,
                   w_gate, w_up, w_down, gain_final, w_vocab):
        L, B, S, KH, HD = k_cache.shape
        D = x_embed.shape[1]
        C = KH * HD
        FF = w_gate.shape[2]
        V = w_vocab.shape[1]
        span = parent.shape[1] // B
        half = HD // 2
        freq = np.power(ROPE_BASE, -(np.arange(half, dtype=np.float64) / half)).astype(np.float32)
        freq = jnp.asarray(np.tile(freq, 2 * KH)[None])
        flat = lambda c: jnp.transpose(c, (0, 1, 3, 4, 2)).reshape(L, B, C, S)
        cfg = (L, B, D, HD, S, KH, FF, V, n_model, span)
        any_spec = pl.BlockSpec(memory_space=pl.ANY)
        vm = pl.BlockSpec(memory_space=pltpu.VMEM)
        sm = pl.BlockSpec(memory_space=pltpu.SMEM)
        steps = 2 * L
        TN = C
        NT = -(-V // TN)
        dma = pltpu.SemaphoreType.DMA
        cache_shape = (L, B, C, S)
        scratch = ([pltpu.VMEM((span * B, C, S), BF16) for _ in range(4)]
                   + [pltpu.VMEM((2, D, C), BF16)] * 3 + [pltpu.VMEM((2, C, D), BF16)]
                   + [pltpu.VMEM((2, D, FF), BF16)] * 2 + [pltpu.VMEM((2, FF, D), BF16)]
                   + [pltpu.VMEM((steps * n_model, B, D), F32), pltpu.VMEM((n_model, 2, B, LANES), F32), pltpu.VMEM((2, SUB, LANES), F32),
                      pltpu.VMEM((B, D), F32), pltpu.VMEM((B, C), F32), pltpu.VMEM((B * SUB, S), F32), pltpu.VMEM((B * SUB, S), F32),
                      pltpu.VMEM((B, C), F32), pltpu.VMEM((NT, B, TN), F32),
                      dma((2 * L,)), dma((14,)), dma((D // S * NT,)), pltpu.SemaphoreType.REGULAR, dma((2 * L,)), dma((2 * L,)),
                      dma((steps * (n_model - 1),)), dma((steps * (n_model - 1),)), dma((n_model - 1,)), dma((n_model - 1,)),
                      dma, dma])
        limit = 64 * 1024 * 1024 - 65536
        outs = pl.pallas_call(
            functools.partial(decode_kernel, cfg),
            out_shape=(pltpu.VMEM(cache_shape, BF16), pltpu.VMEM(cache_shape, BF16), pltpu.VMEM((B, V), F32)),
            in_specs=[sm, sm, vm, vm, vm, vm, vm, vm] + [any_spec] * 10,
            out_specs=(vm, vm, vm),
            scratch_shapes=scratch,
            compiler_params=pltpu.CompilerParams(collective_id=0, has_side_effects=True,
                                                 vmem_limit_bytes=limit - 2 * L * B * C * S * 2 - B * (V + LANES) * 4 - (1 << 19)),
            name="decode_step",
        )(parent, position.reshape(1), x_embed, score[None], freq, gain_attn, gain_mlp, gain_final.reshape(D // LANES, LANES),
          flat(k_cache), flat(v_cache), w_query, w_key, w_value, w_out, w_gate, w_up, w_down, w_vocab.T)
        k_out, v_out, cand = pl.pallas_call(
            write_kernel,
            out_shape=(jax.ShapeDtypeStruct(cache_shape, BF16), jax.ShapeDtypeStruct(cache_shape, BF16),
                       jax.ShapeDtypeStruct((B, V), F32)),
            in_specs=[vm, vm, vm],
            out_specs=(any_spec, any_spec, any_spec),
            scratch_shapes=[dma((2 * L + 1,))],
            compiler_params=pltpu.CompilerParams(vmem_limit_bytes=1 << 20),
            name="write_out",
        )(*outs)
        back = lambda c: jnp.transpose(c.reshape(L, B, KH, HD, S), (0, 1, 4, 2, 3))
        return back(k_out), back(v_out), cand

    return jax.shard_map(local_step, mesh=mesh, in_specs=in_specs, out_specs=out_specs, check_vma=False)
```

```python
import functools

import jax
import jax.numpy as jnp
import numpy as np
from jax import lax
from jax.experimental import pallas as pl
from jax.experimental.pallas import tpu as pltpu
from jax.sharding import PartitionSpec as P

NORM_EPS = 1e-6
ROPE_BASE = 10000.0
MESH = pl.DeviceIdType.MESH
F32 = jnp.float32
BF16 = jnp.bfloat16
LANES = 128
SUB = 8


def rms(res, gain):
    inv = lax.rsqrt(jnp.mean(res * res, axis=-1, keepdims=True) + NORM_EPS)
    return (res * inv * gain.astype(F32)).astype(BF16)


def dot(a, b):
    return jnp.dot(a, b, preferred_element_type=F32)


def dot_t(a, b):
    return lax.dot_general(a, b, (((1,), (1,)), ((), ())), preferred_element_type=F32)


def decode_kernel(cfg, *refs):
    L, B, D, HD, S, KH, FF, V, NM, SPAN = cfg
    (parent_ref, pos_ref, x_ref, score_ref, freq_ref, ga_ref, gm_ref, gf_ref,
     kc, vc, wq, wk, wv, wo, wg, wu, wd, wt, kst, vst, cand_ref,
     kb0, kb1, vb0, vb1, wqb, wkb, wvb, wob, wgb, wub, wdb, ar, stat, scb, res, qs, lg, pr, osc, lgt,
     sem_c, sem_w, sem_t, free, bsend, brecv, asend, arecv, ssend, srecv, csend, crecv) = refs
    kb = (kb0, kb1)
    vb = (vb0, vb1)
    C = KH * HD
    NH, HB = res.shape[:2]
    me = lax.axis_index("model")
    beam = lax.axis_index("beam")
    spos = lax.rem(beam, SPAN)
    sent = lax.div(beam, SPAN)
    partner = beam - spos + lax.rem(spos + 1, SPAN)
    own = pl.ds(spos * B, B)

    def cache_local(l):
        return (pltpu.make_async_copy(kc.at[l], kb[l % 2].at[own], sem_c.at[2 * l]),
                pltpu.make_async_copy(vc.at[l], vb[l % 2].at[own], sem_c.at[2 * l + 1]))

    def cache_push(l):
        return tuple(pltpu.make_async_remote_copy(src_ref=c.at[l], dst_ref=buf[l % 2].at[own], send_sem=bsend.at[2 * l + i],
                                                  recv_sem=brecv.at[2 * l + i], device_id={"beam": partner}, device_id_type=MESH)
                     for i, (c, buf) in enumerate(((kc, kb), (vc, vb))))

    weights = ((wq, wqb), (wk, wkb), (wv, wvb), (wo, wob), (wg, wgb), (wu, wub), (wd, wdb))

    def weight(l, i):
        src, buf = weights[i]
        return pltpu.make_async_copy(src.at[l], buf.at[l % 2], sem_w.at[(l % 2) * 7 + i])

    chunks = (kb0, vb0, kb1, vb1)
    NCH = D // S
    NT = lgt.shape[0]
    TN = lgt.shape[2]

    def vocab(c, n, rows=TN):
        start = n * TN if isinstance(n, int) else pl.multiple_of(n * TN, TN)
        return pltpu.make_async_copy(wt.at[pl.ds(start, rows), c * S:(c + 1) * S], chunks[c].at[n, pl.ds(0, rows)],
                                     sem_t.at[c * NT + n])

    def vocab_all(which, act):
        def body(n, carry):
            for c in which:
                act(vocab(c, n))
            return carry
        full = V // TN
        lax.fori_loop(0, full, body, 0)
        if full < NT:
            for c in which:
                act(vocab(c, full, V - full * TN))

    for i in range(3):
        weight(0, i).start()
    for c in cache_local(0):
        c.start()

    barrier = pltpu.get_barrier_semaphore()
    for k in range(1, NM):
        pl.semaphore_signal(barrier, inc=1, device_id={"model": lax.rem(me + k, NM)}, device_id_type=MESH)
    pl.semaphore_signal(barrier, inc=1, device_id={"beam": partner}, device_id_type=MESH)

    scb[0] = jnp.zeros((SUB, LANES), F32)
    scb[0, 0:1, 0:B] = score_ref[...]
    pos = pos_ref[0]
    angle = pos.astype(F32) * freq_ref[...]
    cos = jnp.cos(angle)
    sin = jnp.sin(angle)
    low = lax.rem(lax.broadcasted_iota(jnp.int32, (HB, C), 1), HD) < HD // 2
    rows = [lax.rem(parent_ref[sent, spos * B + b], SPAN * B) for b in range(B)]

    pl.semaphore_wait(barrier, NM)

    for c in cache_push(0):
        c.start()
    score_copy = pltpu.make_async_remote_copy(src_ref=scb.at[0], dst_ref=scb.at[1], send_sem=csend, recv_sem=crecv,
                                              device_id={"beam": partner}, device_id_type=MESH)
    score_copy.start()
    for i in range(3, 7):
        weight(0, i).start()
    for i in range(7):
        weight(1, i).start()

    def peers():
        if NM == 4:
            return [(3, NM - 1 - me), (2, lax.rem(me + 2, NM)), (1, me + 1 - 2 * lax.rem(me, 2))]
        return [(k, lax.rem(me + k, NM)) for k in range(1, NM)]

    def reduce_start(step, value):
        slot = step * NM + me
        ar[slot] = value
        copies = [pltpu.make_async_remote_copy(src_ref=ar.at[slot], dst_ref=ar.at[slot], send_sem=asend.at[step * (NM - 1) + k - 1],
                                               recv_sem=arecv.at[step * (NM - 1) + k - 1],
                                               device_id={"model": peer}, device_id_type=MESH) for k, peer in peers()]
        for c in copies:
            c.start()
        sends.extend(copies)
        return step, copies

    def reduce_finish(started):
        step, copies = started
        for c in copies:
            c.wait_recv()
        total = ar[step * NM]
        for k in range(1, NM):
            total = total + ar[step * NM + k]
        return total

    def rope(x):
        other = jnp.where(low, -pltpu.roll(x, C - HD // 2, 1), pltpu.roll(x, HD // 2, 1))
        return x * cos + other * sin

    head_of_lane = lax.broadcasted_iota(jnp.int32, (SUB, C), 1) // HD
    head_mask = head_of_lane == lax.broadcasted_iota(jnp.int32, (SUB, C), 0)
    here = lax.broadcasted_iota(jnp.int32, (C, S), 1) == pos
    sends = [score_copy]
    pushes = [cache_push(0)]
    sends.extend(pushes[0])

    def attend(l, i, r):
        ws = l % 2
        h = rms(r, ga_ref[l:l + 1, :])
        if i == 0:
            for j in range(3):
                weight(l, j).wait()
        q = rope(dot(h, wqb[ws])).astype(BF16).astype(F32)
        k = rope(dot(h, wkb[ws])).astype(BF16).astype(F32)
        v = dot(h, wvb[ws]).astype(BF16).astype(F32)
        qs[i] = q * (HD ** -0.5)
        pad = jnp.zeros((LANES - HB, C), F32)
        k_cols = jnp.concatenate([k, pad], axis=0).T
        v_cols = jnp.concatenate([v, pad], axis=0).T
        if i == 0:
            cache_local(l)[0].wait()
            pushes[l][0].wait_recv()
        for b in range(HB):
            kept = jnp.where(here, jnp.broadcast_to(k_cols[:, b:b + 1], (C, S)).astype(BF16), kb[ws][rows[i * HB + b]])
            kst[l, i * HB + b] = kept
            qb = jnp.where(head_mask, jnp.broadcast_to(qs[i, b:b + 1, :], (SUB, C)), 0.0).astype(BF16)
            lg[i, b * SUB:(b + 1) * SUB, :] = dot(qb, kept)
        logits = lg[i]
        logits = jnp.where(lax.broadcasted_iota(jnp.int32, logits.shape, 1) <= pos, logits, -jnp.inf)
        e = jnp.exp(logits - jnp.max(logits, axis=-1, keepdims=True))
        pr[i] = e / jnp.sum(e, axis=-1, keepdims=True)
        if i == 0:
            cache_local(l)[1].wait()
            pushes[l][1].wait_recv()
        for b in range(HB):
            kept = jnp.where(here, jnp.broadcast_to(v_cols[:, b:b + 1], (C, S)).astype(BF16), vb[ws][rows[i * HB + b]])
            vst[l, i * HB + b] = kept
            ob = dot_t(pr[i, b * SUB:(b + 1) * SUB, :].astype(BF16), kept)
            osc[i, b:b + 1, :] = jnp.sum(jnp.where(head_mask, ob, 0.0), axis=0, keepdims=True)
        if i == 0:
            weight(l, 3).wait()
        return reduce_start(2 * l * NH + i, dot(osc[i].astype(BF16), wob[ws]))

    def mlp(l, i, r):
        ws = l % 2
        h = rms(r, gm_ref[l:l + 1, :])
        if i == 0:
            weight(l, 4).wait()
            weight(l, 5).wait()
        gate = dot(h, wgb[ws])
        up = dot(h, wub[ws])
        g = (gate * jax.nn.sigmoid(gate) * up).astype(BF16)
        if i == 0:
            weight(l, 6).wait()
        return reduce_start((2 * l + 1) * NH + i, dot(g, wdb[ws]))

    for i in range(NH):
        res[i] = x_ref[i * HB:(i + 1) * HB, :].astype(F32)
    started = [None] * NH
    for l in range(L):
        for i in range(NH):
            if l > 0:
                res[i] = res[i] + reduce_finish(started[i])
            started[i] = attend(l, i, res[i])
        if l + 2 < L:
            pl.semaphore_signal(free, inc=1, device_id={"beam": partner}, device_id_type=MESH)
        if l + 1 < L:
            if l + 1 >= 2:
                pl.semaphore_wait(free, 1)
            pushes.append(cache_push(l + 1))
            sends.extend(pushes[l + 1])
            pushes[l + 1][0].start()
            for c in cache_local(l + 1):
                c.start()
        if l + 2 < L:
            for j in range(4):
                weight(l + 2, j).start()
        if l == L - 1:
            vocab_all(range(NCH), lambda c: c.start())
        for i in range(NH):
            res[i] = res[i] + reduce_finish(started[i])
            started[i] = mlp(l, i, res[i])
        if l + 1 < L:
            pushes[l + 1][1].start()
        if l + 2 < L:
            for j in range(4, 7):
                weight(l + 2, j).start()
    for i in range(NH):
        res[i] = res[i] + reduce_finish(started[i])

    gf = gf_ref[...].astype(F32)
    h = rms(jnp.concatenate([res[i] for i in range(NH)], axis=0), jnp.concatenate([gf[i:i + 1, :] for i in range(D // LANES)], axis=1))
    vocab_all(range(NCH), lambda c: c.wait())

    def tile(n, carry):
        acc = dot_t(h[:, 0:S], chunks[0][n])
        for c in range(1, NCH):
            acc = acc + dot_t(h[:, c * S:(c + 1) * S], chunks[c][n])
        acc = jnp.where(lax.broadcasted_iota(jnp.int32, (B, TN), 1) + n * TN < V, acc, -jnp.inf)
        lgt[n] = acc
        return jnp.maximum(carry, acc)

    peak = lax.fori_loop(0, NT, tile, jnp.full((B, TN), -jnp.inf, F32))
    m = jnp.max(peak, axis=-1, keepdims=True)

    def add_exp(n, carry):
        return carry + jnp.exp(lgt[n] - m)

    s = jnp.sum(lax.fori_loop(0, NT, add_exp, jnp.zeros((B, TN), F32)), axis=-1, keepdims=True)
    stat[me, 0] = jnp.broadcast_to(m, (B, LANES))
    stat[me, 1] = jnp.broadcast_to(s, (B, LANES))
    copies = [pltpu.make_async_remote_copy(src_ref=stat.at[me], dst_ref=stat.at[me], send_sem=ssend.at[k - 1], recv_sem=srecv.at[k - 1],
                                           device_id={"model": lax.rem(me + k, NM)}, device_id_type=MESH) for k in range(1, NM)]
    for c in copies:
        c.start()
    sends += copies
    score_copy.wait_recv()
    sub = lax.broadcasted_iota(jnp.int32, (B, LANES), 0)
    want = jnp.zeros((B, LANES), jnp.int32)
    for b in range(B):
        want = jnp.where(sub == b, rows[b], want)
    lane = lax.broadcasted_iota(jnp.int32, (B, LANES), 1)
    mine = jnp.where(lane + spos * B == want, scb[0, 0:1, :], 0.0)
    theirs = jnp.where(lane + (SPAN - 1 - spos) * B == want, scb[1, 0:1, :], 0.0)
    parent_score = jnp.sum(jnp.where(lane < B, mine + theirs, 0.0), axis=-1, keepdims=True)
    for c in copies:
        c.wait_recv()
    gm = stat[0, 0]
    for k in range(1, NM):
        gm = jnp.maximum(gm, stat[k, 0])
    gs = stat[0, 1] * jnp.exp(stat[0, 0] - gm)
    for k in range(1, NM):
        gs = gs + stat[k, 1] * jnp.exp(stat[k, 0] - gm)
    gm = gm[:, 0:1]
    log_s = jnp.log(gs)[:, 0:1]
    for n in range(NT):
        hi = min((n + 1) * TN, V)
        cand_ref[:, n * TN:hi] = parent_score + ((lgt[n] - gm) - log_s)[:, :hi - n * TN]
    for c in sends:
        c.wait_send()


def write_kernel(*refs):
    n = (len(refs) - 1) // 2
    sem = refs[-1]
    copies = []
    for i in range(n):
        src, dst = refs[i], refs[n + i]
        if len(src.shape) > 2:
            copies += [(src.at[j], dst.at[j]) for j in range(src.shape[0])]
        else:
            copies.append((src, dst))
    copies = [pltpu.make_async_copy(a, b, sem.at[j]) for j, (a, b) in enumerate(copies)]
    for c in copies:
        c.start()
    for c in copies:
        c.wait()


def solution(mesh):
    data_beam = ('data', 'beam')
    cache_spec = P(None, data_beam, None, 'model', None)
    col_spec = P(None, None, 'model')
    row_spec = P(None, 'model', None)
    in_specs = (P(data_beam, None), P('data', None), P(), P(data_beam), cache_spec, cache_spec,
                P(), col_spec, col_spec, col_spec, row_spec, P(), col_spec, col_spec, row_spec, P(), P(None, 'model'))
    out_specs = (cache_spec, cache_spec, P(data_beam, 'model'))
    n_model = mesh.shape['model']

    def local_step(x_embed, parent, position, score, k_cache, v_cache, gain_attn, w_query, w_key, w_value, w_out, gain_mlp,
                   w_gate, w_up, w_down, gain_final, w_vocab):
        L, B, S, KH, HD = k_cache.shape
        D = x_embed.shape[1]
        C = KH * HD
        FF = w_gate.shape[2]
        V = w_vocab.shape[1]
        span = parent.shape[1] // B
        half = HD // 2
        freq = np.power(ROPE_BASE, -(np.arange(half, dtype=np.float64) / half)).astype(np.float32)
        freq = jnp.asarray(np.tile(freq, 2 * KH)[None])
        flat = lambda c: jnp.transpose(c, (0, 1, 3, 4, 2)).reshape(L, B, C, S)
        cfg = (L, B, D, HD, S, KH, FF, V, n_model, span)
        any_spec = pl.BlockSpec(memory_space=pl.ANY)
        vm = pl.BlockSpec(memory_space=pltpu.VMEM)
        sm = pl.BlockSpec(memory_space=pltpu.SMEM)
        steps = 2 * L
        NH = 2
        HB = B // NH
        TN = C
        NT = -(-V // TN)
        dma = pltpu.SemaphoreType.DMA
        cache_shape = (L, B, C, S)
        scratch = ([pltpu.VMEM((span * B, C, S), BF16) for _ in range(4)]
                   + [pltpu.VMEM((2, D, C), BF16)] * 3 + [pltpu.VMEM((2, C, D), BF16)]
                   + [pltpu.VMEM((2, D, FF), BF16)] * 2 + [pltpu.VMEM((2, FF, D), BF16)]
                   + [pltpu.VMEM((steps * NH * n_model, HB, D), F32), pltpu.VMEM((n_model, 2, B, LANES), F32), pltpu.VMEM((2, SUB, LANES), F32),
                      pltpu.VMEM((NH, HB, D), F32), pltpu.VMEM((NH, HB, C), F32), pltpu.VMEM((NH, HB * SUB, S), F32),
                      pltpu.VMEM((NH, HB * SUB, S), F32), pltpu.VMEM((NH, HB, C), F32), pltpu.VMEM((NT, B, TN), F32),
                      dma((2 * L,)), dma((14,)), dma((D // S * NT,)), pltpu.SemaphoreType.REGULAR, dma((2 * L,)), dma((2 * L,)),
                      dma((steps * NH * (n_model - 1),)), dma((steps * NH * (n_model - 1),)), dma((n_model - 1,)), dma((n_model - 1,)),
                      dma, dma])
        limit = 64 * 1024 * 1024 - 65536
        outs = pl.pallas_call(
            functools.partial(decode_kernel, cfg),
            out_shape=(pltpu.VMEM(cache_shape, BF16), pltpu.VMEM(cache_shape, BF16), pltpu.VMEM((B, V), F32)),
            in_specs=[sm, sm, vm, vm, vm, vm, vm, vm] + [any_spec] * 10,
            out_specs=(vm, vm, vm),
            scratch_shapes=scratch,
            compiler_params=pltpu.CompilerParams(collective_id=0, has_side_effects=True,
                                                 vmem_limit_bytes=limit - 2 * L * B * C * S * 2 - B * (V + LANES) * 4 - (1 << 19)),
            name="decode_step",
        )(parent, position.reshape(1), x_embed, score[None], freq, gain_attn, gain_mlp, gain_final.reshape(D // LANES, LANES),
          flat(k_cache), flat(v_cache), w_query, w_key, w_value, w_out, w_gate, w_up, w_down, w_vocab.T)
        k_out, v_out, cand = pl.pallas_call(
            write_kernel,
            out_shape=(jax.ShapeDtypeStruct(cache_shape, BF16), jax.ShapeDtypeStruct(cache_shape, BF16),
                       jax.ShapeDtypeStruct((B, V), F32)),
            in_specs=[vm, vm, vm],
            out_specs=(any_spec, any_spec, any_spec),
            scratch_shapes=[dma((2 * L + 1,))],
            compiler_params=pltpu.CompilerParams(vmem_limit_bytes=1 << 20),
            name="write_out",
        )(*outs)
        back = lambda c: jnp.transpose(c.reshape(L, B, KH, HD, S), (0, 1, 4, 2, 3))
        return back(k_out), back(v_out), cand

    return jax.shard_map(local_step, mesh=mesh, in_specs=in_specs, out_specs=out_specs, check_vma=False)
```

```python
import functools

import jax
import jax.numpy as jnp
import numpy as np
from jax import lax
from jax.experimental import pallas as pl
from jax.experimental.pallas import tpu as pltpu
from jax.sharding import PartitionSpec as P

NORM_EPS = 1e-6
ROPE_BASE = 10000.0
MESH = pl.DeviceIdType.MESH
F32 = jnp.float32
BF16 = jnp.bfloat16
LANES = 128
SUB = 8


def rms(res, gain):
    inv = lax.rsqrt(jnp.mean(res * res, axis=-1, keepdims=True) + NORM_EPS)
    return (res * inv * gain.astype(F32)).astype(BF16)


def dot(a, b):
    return jnp.dot(a, b, preferred_element_type=F32)


def dot_t(a, b):
    return lax.dot_general(a, b, (((1,), (1,)), ((), ())), preferred_element_type=F32)


def decode_kernel(cfg, *refs):
    L, B, D, HD, S, KH, FF, V, NM, SPAN = cfg
    (parent_ref, pos_ref, x_ref, score_ref, freq_ref, ga_ref, gm_ref, gf_ref,
     kc, vc, wq, wk, wv, wo, wg, wu, wd, wt, kst, vst, cand_ref,
     kb0, kb1, vb0, vb1, wqb, wkb, wvb, wob, wgb, wub, wdb, ar, stat, scb, res, qs, lg, pr, osc, lgt,
     sem_c, sem_w, sem_t, free, bsend, brecv, asend, arecv, ssend, srecv, csend, crecv) = refs
    kb = (kb0, kb1)
    vb = (vb0, vb1)
    C = KH * HD
    NH, HB = res.shape[:2]
    me = lax.axis_index("model")
    beam = lax.axis_index("beam")
    spos = lax.rem(beam, SPAN)
    sent = lax.div(beam, SPAN)
    partner = beam - spos + lax.rem(spos + 1, SPAN)
    own = pl.ds(spos * B, B)

    def cache_local(l):
        return (pltpu.make_async_copy(kc.at[l], kb[l % 2].at[own], sem_c.at[2 * l]),
                pltpu.make_async_copy(vc.at[l], vb[l % 2].at[own], sem_c.at[2 * l + 1]))

    def cache_push(l):
        return tuple(pltpu.make_async_remote_copy(src_ref=c.at[l], dst_ref=buf[l % 2].at[own], send_sem=bsend.at[2 * l + i],
                                                  recv_sem=brecv.at[2 * l + i], device_id={"beam": partner}, device_id_type=MESH)
                     for i, (c, buf) in enumerate(((kc, kb), (vc, vb))))

    weights = ((wq, wqb), (wk, wkb), (wv, wvb), (wo, wob), (wg, wgb), (wu, wub), (wd, wdb))

    def weight(l, i):
        src, buf = weights[i]
        return pltpu.make_async_copy(src.at[l], buf.at[l % 2], sem_w.at[(l % 2) * 7 + i])

    chunks = (kb0, vb0, kb1, vb1)
    NCH = D // S
    NT = lgt.shape[0]
    TN = lgt.shape[2]

    def vocab(c, n, rows=TN):
        start = n * TN if isinstance(n, int) else pl.multiple_of(n * TN, TN)
        return pltpu.make_async_copy(wt.at[pl.ds(start, rows), c * S:(c + 1) * S], chunks[c].at[n, pl.ds(0, rows)],
                                     sem_t.at[c * NT + n])

    def vocab_all(which, act):
        def body(n, carry):
            for c in which:
                act(vocab(c, n))
            return carry
        full = V // TN
        lax.fori_loop(0, full, body, 0)
        if full < NT:
            for c in which:
                act(vocab(c, full, V - full * TN))

    for i in range(3):
        weight(0, i).start()
    for c in cache_local(0):
        c.start()

    barrier = pltpu.get_barrier_semaphore()
    for k in range(1, NM):
        pl.semaphore_signal(barrier, inc=1, device_id={"model": lax.rem(me + k, NM)}, device_id_type=MESH)
    pl.semaphore_signal(barrier, inc=1, device_id={"beam": partner}, device_id_type=MESH)

    scb[0] = jnp.zeros((SUB, LANES), F32)
    scb[0, 0:1, 0:B] = score_ref[...]
    pos = pos_ref[0]
    angle = pos.astype(F32) * freq_ref[...]
    cos = jnp.cos(angle)
    sin = jnp.sin(angle)
    low = lax.rem(lax.broadcasted_iota(jnp.int32, (HB, C), 1), HD) < HD // 2
    rows = [lax.rem(parent_ref[sent, spos * B + b], SPAN * B) for b in range(B)]

    pl.semaphore_wait(barrier, NM)

    for c in cache_push(0):
        c.start()
    score_copy = pltpu.make_async_remote_copy(src_ref=scb.at[0], dst_ref=scb.at[1], send_sem=csend, recv_sem=crecv,
                                              device_id={"beam": partner}, device_id_type=MESH)
    score_copy.start()
    for i in range(3, 7):
        weight(0, i).start()
    for i in range(7):
        weight(1, i).start()

    def peers():
        if NM == 4:
            side = lax.div(me, 2)
            return [3 - 3 * side, 2 - side, me + 1 - 2 * lax.rem(me, 2)]
        return [lax.rem(me + k, NM) for k in range(1, NM)]

    def reduce_copy(step, j, source, peer):
        slot = step * NM + source
        return pltpu.make_async_remote_copy(src_ref=ar.at[slot], dst_ref=ar.at[slot], send_sem=asend.at[step * (NM - 1) + j],
                                            recv_sem=arecv.at[slot], device_id={"model": peer}, device_id_type=MESH)

    def reduce_start(step, value):
        ar[step * NM + me] = value
        copies = [reduce_copy(step, j, me, peer) for j, peer in enumerate(peers())]
        for c in copies:
            c.start()
        sends.extend(copies)
        return step

    def reduce_finish(step):
        for k in range(1, NM):
            reduce_copy(step, 0, lax.rem(me + k, NM), me).wait_recv()
        total = ar[step * NM]
        for k in range(1, NM):
            total = total + ar[step * NM + k]
        return total

    def rope(x):
        other = jnp.where(low, -pltpu.roll(x, C - HD // 2, 1), pltpu.roll(x, HD // 2, 1))
        return x * cos + other * sin

    head_of_lane = lax.broadcasted_iota(jnp.int32, (SUB, C), 1) // HD
    head_mask = head_of_lane == lax.broadcasted_iota(jnp.int32, (SUB, C), 0)
    here = lax.broadcasted_iota(jnp.int32, (C, S), 1) == pos
    sends = [score_copy]
    pushes = [cache_push(0)]
    sends.extend(pushes[0])

    def attend(l, i, r):
        ws = l % 2
        h = rms(r, ga_ref[l:l + 1, :])
        if i == 0:
            for j in range(3):
                weight(l, j).wait()
        q = rope(dot(h, wqb[ws])).astype(BF16).astype(F32)
        k = rope(dot(h, wkb[ws])).astype(BF16).astype(F32)
        v = dot(h, wvb[ws]).astype(BF16).astype(F32)
        qs[i] = q * (HD ** -0.5)
        pad = jnp.zeros((LANES - HB, C), F32)
        k_cols = jnp.concatenate([k, pad], axis=0).T
        v_cols = jnp.concatenate([v, pad], axis=0).T
        if i == 0:
            cache_local(l)[0].wait()
            pushes[l][0].wait_recv()
        for b in range(HB):
            kept = jnp.where(here, jnp.broadcast_to(k_cols[:, b:b + 1], (C, S)).astype(BF16), kb[ws][rows[i * HB + b]])
            kst[l, i * HB + b] = kept
            qb = jnp.where(head_mask, jnp.broadcast_to(qs[i, b:b + 1, :], (SUB, C)), 0.0).astype(BF16)
            lg[i, b * SUB:(b + 1) * SUB, :] = dot(qb, kept)
        logits = lg[i]
        logits = jnp.where(lax.broadcasted_iota(jnp.int32, logits.shape, 1) <= pos, logits, -jnp.inf)
        e = jnp.exp(logits - jnp.max(logits, axis=-1, keepdims=True))
        pr[i] = e / jnp.sum(e, axis=-1, keepdims=True)
        if i == 0:
            cache_local(l)[1].wait()
            pushes[l][1].wait_recv()
        for b in range(HB):
            kept = jnp.where(here, jnp.broadcast_to(v_cols[:, b:b + 1], (C, S)).astype(BF16), vb[ws][rows[i * HB + b]])
            vst[l, i * HB + b] = kept
            ob = dot_t(pr[i, b * SUB:(b + 1) * SUB, :].astype(BF16), kept)
            osc[i, b:b + 1, :] = jnp.sum(jnp.where(head_mask, ob, 0.0), axis=0, keepdims=True)
        if i == 0:
            weight(l, 3).wait()
        return reduce_start(2 * l * NH + i, dot(osc[i].astype(BF16), wob[ws]))

    def mlp(l, i, r):
        ws = l % 2
        h = rms(r, gm_ref[l:l + 1, :])
        if i == 0:
            weight(l, 4).wait()
            weight(l, 5).wait()
        gate = dot(h, wgb[ws])
        up = dot(h, wub[ws])
        g = (gate * jax.nn.sigmoid(gate) * up).astype(BF16)
        if i == 0:
            weight(l, 6).wait()
        return reduce_start((2 * l + 1) * NH + i, dot(g, wdb[ws]))

    for i in range(NH):
        res[i] = x_ref[i * HB:(i + 1) * HB, :].astype(F32)
    started = [None] * NH
    for l in range(L):
        for i in range(NH):
            if l > 0:
                res[i] = res[i] + reduce_finish(started[i])
            started[i] = attend(l, i, res[i])
        if l + 2 < L:
            pl.semaphore_signal(free, inc=1, device_id={"beam": partner}, device_id_type=MESH)
        if l + 1 < L:
            if l + 1 >= 2:
                pl.semaphore_wait(free, 1)
            pushes.append(cache_push(l + 1))
            sends.extend(pushes[l + 1])
            pushes[l + 1][0].start()
            for c in cache_local(l + 1):
                c.start()
        if l + 2 < L:
            for j in range(4):
                weight(l + 2, j).start()
        if l == L - 1:
            vocab_all(range(NCH), lambda c: c.start())
        for i in range(NH):
            res[i] = res[i] + reduce_finish(started[i])
            started[i] = mlp(l, i, res[i])
        if l + 1 < L:
            pushes[l + 1][1].start()
        if l + 2 < L:
            for j in range(4, 7):
                weight(l + 2, j).start()
    for i in range(NH):
        res[i] = res[i] + reduce_finish(started[i])

    gf = gf_ref[...].astype(F32)
    h = rms(jnp.concatenate([res[i] for i in range(NH)], axis=0), jnp.concatenate([gf[i:i + 1, :] for i in range(D // LANES)], axis=1))
    vocab_all(range(NCH), lambda c: c.wait())

    def tile(n, carry):
        acc = dot_t(h[:, 0:S], chunks[0][n])
        for c in range(1, NCH):
            acc = acc + dot_t(h[:, c * S:(c + 1) * S], chunks[c][n])
        acc = jnp.where(lax.broadcasted_iota(jnp.int32, (B, TN), 1) + n * TN < V, acc, -jnp.inf)
        lgt[n] = acc
        return jnp.maximum(carry, acc)

    peak = lax.fori_loop(0, NT, tile, jnp.full((B, TN), -jnp.inf, F32))
    m = jnp.max(peak, axis=-1, keepdims=True)

    def add_exp(n, carry):
        return carry + jnp.exp(lgt[n] - m)

    s = jnp.sum(lax.fori_loop(0, NT, add_exp, jnp.zeros((B, TN), F32)), axis=-1, keepdims=True)
    stat[me, 0] = jnp.broadcast_to(m, (B, LANES))
    stat[me, 1] = jnp.broadcast_to(s, (B, LANES))
    copies = [pltpu.make_async_remote_copy(src_ref=stat.at[me], dst_ref=stat.at[me], send_sem=ssend.at[k - 1], recv_sem=srecv.at[k - 1],
                                           device_id={"model": lax.rem(me + k, NM)}, device_id_type=MESH) for k in range(1, NM)]
    for c in copies:
        c.start()
    sends += copies
    score_copy.wait_recv()
    sub = lax.broadcasted_iota(jnp.int32, (B, LANES), 0)
    want = jnp.zeros((B, LANES), jnp.int32)
    for b in range(B):
        want = jnp.where(sub == b, rows[b], want)
    lane = lax.broadcasted_iota(jnp.int32, (B, LANES), 1)
    mine = jnp.where(lane + spos * B == want, scb[0, 0:1, :], 0.0)
    theirs = jnp.where(lane + (SPAN - 1 - spos) * B == want, scb[1, 0:1, :], 0.0)
    parent_score = jnp.sum(jnp.where(lane < B, mine + theirs, 0.0), axis=-1, keepdims=True)
    for c in copies:
        c.wait_recv()
    gm = stat[0, 0]
    for k in range(1, NM):
        gm = jnp.maximum(gm, stat[k, 0])
    gs = stat[0, 1] * jnp.exp(stat[0, 0] - gm)
    for k in range(1, NM):
        gs = gs + stat[k, 1] * jnp.exp(stat[k, 0] - gm)
    gm = gm[:, 0:1]
    log_s = jnp.log(gs)[:, 0:1]
    for n in range(NT):
        hi = min((n + 1) * TN, V)
        cand_ref[:, n * TN:hi] = parent_score + ((lgt[n] - gm) - log_s)[:, :hi - n * TN]
    for c in sends:
        c.wait_send()


def write_kernel(*refs):
    n = (len(refs) - 1) // 2
    sem = refs[-1]
    copies = []
    for i in range(n):
        src, dst = refs[i], refs[n + i]
        if len(src.shape) > 2:
            copies += [(src.at[j], dst.at[j]) for j in range(src.shape[0])]
        else:
            copies.append((src, dst))
    copies = [pltpu.make_async_copy(a, b, sem.at[j]) for j, (a, b) in enumerate(copies)]
    for c in copies:
        c.start()
    for c in copies:
        c.wait()


def solution(mesh):
    data_beam = ('data', 'beam')
    cache_spec = P(None, data_beam, None, 'model', None)
    col_spec = P(None, None, 'model')
    row_spec = P(None, 'model', None)
    in_specs = (P(data_beam, None), P('data', None), P(), P(data_beam), cache_spec, cache_spec,
                P(), col_spec, col_spec, col_spec, row_spec, P(), col_spec, col_spec, row_spec, P(), P(None, 'model'))
    out_specs = (cache_spec, cache_spec, P(data_beam, 'model'))
    n_model = mesh.shape['model']

    def local_step(x_embed, parent, position, score, k_cache, v_cache, gain_attn, w_query, w_key, w_value, w_out, gain_mlp,
                   w_gate, w_up, w_down, gain_final, w_vocab):
        L, B, S, KH, HD = k_cache.shape
        D = x_embed.shape[1]
        C = KH * HD
        FF = w_gate.shape[2]
        V = w_vocab.shape[1]
        span = parent.shape[1] // B
        half = HD // 2
        freq = np.power(ROPE_BASE, -(np.arange(half, dtype=np.float64) / half)).astype(np.float32)
        freq = jnp.asarray(np.tile(freq, 2 * KH)[None])
        flat = lambda c: jnp.transpose(c, (0, 1, 3, 4, 2)).reshape(L, B, C, S)
        cfg = (L, B, D, HD, S, KH, FF, V, n_model, span)
        any_spec = pl.BlockSpec(memory_space=pl.ANY)
        vm = pl.BlockSpec(memory_space=pltpu.VMEM)
        sm = pl.BlockSpec(memory_space=pltpu.SMEM)
        steps = 2 * L
        NH = 4
        HB = B // NH
        TN = C
        NT = -(-V // TN)
        dma = pltpu.SemaphoreType.DMA
        cache_shape = (L, B, C, S)
        scratch = ([pltpu.VMEM((span * B, C, S), BF16) for _ in range(4)]
                   + [pltpu.VMEM((2, D, C), BF16)] * 3 + [pltpu.VMEM((2, C, D), BF16)]
                   + [pltpu.VMEM((2, D, FF), BF16)] * 2 + [pltpu.VMEM((2, FF, D), BF16)]
                   + [pltpu.VMEM((steps * NH * n_model, HB, D), F32), pltpu.VMEM((n_model, 2, B, LANES), F32), pltpu.VMEM((2, SUB, LANES), F32),
                      pltpu.VMEM((NH, HB, D), F32), pltpu.VMEM((NH, HB, C), F32), pltpu.VMEM((NH, HB * SUB, S), F32),
                      pltpu.VMEM((NH, HB * SUB, S), F32), pltpu.VMEM((NH, HB, C), F32), pltpu.VMEM((NT, B, TN), F32),
                      dma((2 * L,)), dma((14,)), dma((D // S * NT,)), pltpu.SemaphoreType.REGULAR, dma((2 * L,)), dma((2 * L,)),
                      dma((steps * NH * (n_model - 1),)), dma((steps * NH * n_model,)), dma((n_model - 1,)), dma((n_model - 1,)),
                      dma, dma])
        limit = 64 * 1024 * 1024 - 65536
        outs = pl.pallas_call(
            functools.partial(decode_kernel, cfg),
            out_shape=(pltpu.VMEM(cache_shape, BF16), pltpu.VMEM(cache_shape, BF16), pltpu.VMEM((B, V), F32)),
            in_specs=[sm, sm, vm, vm, vm, vm, vm, vm] + [any_spec] * 10,
            out_specs=(vm, vm, vm),
            scratch_shapes=scratch,
            compiler_params=pltpu.CompilerParams(collective_id=0, has_side_effects=True,
                                                 vmem_limit_bytes=limit - 2 * L * B * C * S * 2 - B * (V + LANES) * 4 - (1 << 19)),
            name="decode_step",
        )(parent, position.reshape(1), x_embed, score[None], freq, gain_attn, gain_mlp, gain_final.reshape(D // LANES, LANES),
          flat(k_cache), flat(v_cache), w_query, w_key, w_value, w_out, w_gate, w_up, w_down, w_vocab.T)
        k_out, v_out, cand = pl.pallas_call(
            write_kernel,
            out_shape=(jax.ShapeDtypeStruct(cache_shape, BF16), jax.ShapeDtypeStruct(cache_shape, BF16),
                       jax.ShapeDtypeStruct((B, V), F32)),
            in_specs=[vm, vm, vm],
            out_specs=(any_spec, any_spec, any_spec),
            scratch_shapes=[dma((2 * L + 1,))],
            compiler_params=pltpu.CompilerParams(vmem_limit_bytes=1 << 20),
            name="write_out",
        )(*outs)
        back = lambda c: jnp.transpose(c.reshape(L, B, KH, HD, S), (0, 1, 4, 2, 3))
        return back(k_out), back(v_out), cand

    return jax.shard_map(local_step, mesh=mesh, in_specs=in_specs, out_specs=out_specs, check_vma=False)
```

```python
import functools

import jax
import jax.numpy as jnp
import numpy as np
from jax import lax
from jax.experimental import pallas as pl
from jax.experimental.pallas import tpu as pltpu
from jax.sharding import PartitionSpec as P

NORM_EPS = 1e-6
ROPE_BASE = 10000.0
MESH = pl.DeviceIdType.MESH
F32 = jnp.float32
BF16 = jnp.bfloat16
LANES = 128
SUB = 8


def rms(res, gain):
    inv = lax.rsqrt(jnp.mean(res * res, axis=-1, keepdims=True) + NORM_EPS)
    return (res * inv * gain.astype(F32)).astype(BF16)


def dot(a, b):
    return jnp.dot(a, b, preferred_element_type=F32)


def dot_t(a, b):
    return lax.dot_general(a, b, (((1,), (1,)), ((), ())), preferred_element_type=F32)


def decode_kernel(cfg, *refs):
    L, B, D, HD, S, KH, FF, V, NM, SPAN = cfg
    (parent_ref, pos_ref, x_ref, score_ref, freq_ref, ga_ref, gm_ref, gf_ref,
     kc, vc, wq, wk, wv, wo, wg, wu, wd, wt, kst, vst, cand_ref,
     kb0, kb1, vb0, vb1, wqb, wkb, wvb, wob, wgb, wub, wdb, ar, stat, scb, res, qs, lg, pr, osc, lgt,
     sem_c, sem_w, sem_t, free, bsend, brecv, asend, arecv, ssend, srecv, csend, crecv) = refs
    kb = (kb0, kb1)
    vb = (vb0, vb1)
    C = KH * HD
    NH, HB = res.shape[:2]
    me = lax.axis_index("model")
    beam = lax.axis_index("beam")
    spos = lax.rem(beam, SPAN)
    sent = lax.div(beam, SPAN)
    partner = beam - spos + lax.rem(spos + 1, SPAN)
    own = pl.ds(spos * B, B)

    def cache_local(l):
        return (pltpu.make_async_copy(kc.at[l], kb[l % 2].at[own], sem_c.at[2 * l]),
                pltpu.make_async_copy(vc.at[l], vb[l % 2].at[own], sem_c.at[2 * l + 1]))

    def cache_push(l):
        return tuple(pltpu.make_async_remote_copy(src_ref=c.at[l], dst_ref=buf[l % 2].at[own], send_sem=bsend.at[2 * l + i],
                                                  recv_sem=brecv.at[2 * l + i], device_id={"beam": partner}, device_id_type=MESH)
                     for i, (c, buf) in enumerate(((kc, kb), (vc, vb))))

    weights = ((wq, wqb), (wk, wkb), (wv, wvb), (wo, wob), (wg, wgb), (wu, wub), (wd, wdb))

    def weight(l, i):
        src, buf = weights[i]
        return pltpu.make_async_copy(src.at[l], buf.at[l % 2], sem_w.at[(l % 2) * 7 + i])

    chunks = (kb0, vb0, kb1, vb1)
    NCH = D // S
    NT = lgt.shape[0]
    TN = lgt.shape[2]

    def vocab(c, n, rows=TN):
        start = n * TN if isinstance(n, int) else pl.multiple_of(n * TN, TN)
        return pltpu.make_async_copy(wt.at[pl.ds(start, rows), c * S:(c + 1) * S], chunks[c].at[n, pl.ds(0, rows)],
                                     sem_t.at[c * NT + n])

    def vocab_all(which, act):
        def body(n, carry):
            for c in which:
                act(vocab(c, n))
            return carry
        full = V // TN
        lax.fori_loop(0, full, body, 0)
        if full < NT:
            for c in which:
                act(vocab(c, full, V - full * TN))

    for i in range(3):
        weight(0, i).start()
    for l in range(2):
        for c in cache_local(l):
            c.start()

    barrier = pltpu.get_barrier_semaphore()
    for k in range(1, NM):
        pl.semaphore_signal(barrier, inc=1, device_id={"model": lax.rem(me + k, NM)}, device_id_type=MESH)
    pl.semaphore_signal(barrier, inc=1, device_id={"beam": partner}, device_id_type=MESH)

    scb[0] = jnp.zeros((SUB, LANES), F32)
    scb[0, 0:1, 0:B] = score_ref[...]
    pos = pos_ref[0]
    angle = pos.astype(F32) * freq_ref[...]
    cos = jnp.cos(angle)
    sin = jnp.sin(angle)
    low = lax.rem(lax.broadcasted_iota(jnp.int32, (HB, C), 1), HD) < HD // 2
    rows = [lax.rem(parent_ref[sent, spos * B + b], SPAN * B) for b in range(B)]

    pl.semaphore_wait(barrier, NM)

    pushes = [cache_push(l) for l in range(L)]
    for c in (pushes[0][0], pushes[0][1], pushes[1][0]):
        c.start()
    score_copy = pltpu.make_async_remote_copy(src_ref=scb.at[0], dst_ref=scb.at[1], send_sem=csend, recv_sem=crecv,
                                              device_id={"beam": partner}, device_id_type=MESH)
    score_copy.start()
    for i in range(3, 7):
        weight(0, i).start()
    for i in range(7):
        weight(1, i).start()

    def peers():
        if NM == 4:
            side = lax.div(me, 2)
            return [3 - 3 * side, 2 - side, me + 1 - 2 * lax.rem(me, 2)]
        return [lax.rem(me + k, NM) for k in range(1, NM)]

    def reduce_copy(step, j, source, peer):
        slot = step * NM + source
        return pltpu.make_async_remote_copy(src_ref=ar.at[slot], dst_ref=ar.at[slot], send_sem=asend.at[step * (NM - 1) + j],
                                            recv_sem=arecv.at[slot], device_id={"model": peer}, device_id_type=MESH)

    def reduce_start(step, value):
        ar[step * NM + me] = value
        copies = [reduce_copy(step, j, me, peer) for j, peer in enumerate(peers())]
        for c in copies:
            c.start()
        sends.extend(copies)
        return step

    def reduce_finish(step):
        for k in range(1, NM):
            reduce_copy(step, 0, lax.rem(me + k, NM), me).wait_recv()
        total = ar[step * NM]
        for k in range(1, NM):
            total = total + ar[step * NM + k]
        return total

    def rope(x):
        other = jnp.where(low, -pltpu.roll(x, C - HD // 2, 1), pltpu.roll(x, HD // 2, 1))
        return x * cos + other * sin

    head_of_lane = lax.broadcasted_iota(jnp.int32, (SUB, C), 1) // HD
    head_mask = head_of_lane == lax.broadcasted_iota(jnp.int32, (SUB, C), 0)
    here = lax.broadcasted_iota(jnp.int32, (C, S), 1) == pos
    sends = [score_copy]
    sends.extend(pushes[l][i] for l in range(L) for i in range(2))

    def attend(l, i, r):
        ws = l % 2
        h = rms(r, ga_ref[l:l + 1, :])
        if i == 0:
            for j in range(3):
                weight(l, j).wait()
        q = rope(dot(h, wqb[ws])).astype(BF16).astype(F32)
        k = rope(dot(h, wkb[ws])).astype(BF16).astype(F32)
        v = dot(h, wvb[ws]).astype(BF16).astype(F32)
        qs[i] = q * (HD ** -0.5)
        pad = jnp.zeros((LANES - HB, C), F32)
        k_cols = jnp.concatenate([k, pad], axis=0).T
        v_cols = jnp.concatenate([v, pad], axis=0).T
        if i == 0:
            cache_local(l)[0].wait()
            pushes[l][0].wait_recv()
        for b in range(HB):
            kept = jnp.where(here, jnp.broadcast_to(k_cols[:, b:b + 1], (C, S)).astype(BF16), kb[ws][rows[i * HB + b]])
            kst[l, i * HB + b] = kept
            qb = jnp.where(head_mask, jnp.broadcast_to(qs[i, b:b + 1, :], (SUB, C)), 0.0).astype(BF16)
            lg[i, b * SUB:(b + 1) * SUB, :] = dot(qb, kept)
        logits = lg[i]
        logits = jnp.where(lax.broadcasted_iota(jnp.int32, logits.shape, 1) <= pos, logits, -jnp.inf)
        e = jnp.exp(logits - jnp.max(logits, axis=-1, keepdims=True))
        pr[i] = e / jnp.sum(e, axis=-1, keepdims=True)
        if i == 0:
            cache_local(l)[1].wait()
            pushes[l][1].wait_recv()
        for b in range(HB):
            kept = jnp.where(here, jnp.broadcast_to(v_cols[:, b:b + 1], (C, S)).astype(BF16), vb[ws][rows[i * HB + b]])
            vst[l, i * HB + b] = kept
            ob = dot_t(pr[i, b * SUB:(b + 1) * SUB, :].astype(BF16), kept)
            osc[i, b:b + 1, :] = jnp.sum(jnp.where(head_mask, ob, 0.0), axis=0, keepdims=True)
        if i == 0:
            weight(l, 3).wait()
        return reduce_start(2 * l * NH + i, dot(osc[i].astype(BF16), wob[ws]))

    def mlp(l, i, r):
        ws = l % 2
        h = rms(r, gm_ref[l:l + 1, :])
        if i == 0:
            weight(l, 4).wait()
            weight(l, 5).wait()
        gate = dot(h, wgb[ws])
        up = dot(h, wub[ws])
        g = (gate * jax.nn.sigmoid(gate) * up).astype(BF16)
        if i == 0:
            weight(l, 6).wait()
        return reduce_start((2 * l + 1) * NH + i, dot(g, wdb[ws]))

    for i in range(NH):
        res[i] = x_ref[i * HB:(i + 1) * HB, :].astype(F32)
    started = [None] * NH
    for l in range(L):
        for i in range(NH):
            if l > 0:
                res[i] = res[i] + reduce_finish(started[i])
            started[i] = attend(l, i, res[i])
        if l + 2 < L:
            pl.semaphore_signal(free, inc=1, device_id={"beam": partner}, device_id_type=MESH)
            for c in cache_local(l + 2):
                c.start()
        if l + 1 < L:
            pushes[l + 1][1].start()
        if l + 2 < L:
            for j in range(4):
                weight(l + 2, j).start()
        if l == L - 1:
            vocab_all(range(NCH), lambda c: c.start())
        for i in range(NH):
            res[i] = res[i] + reduce_finish(started[i])
            started[i] = mlp(l, i, res[i])
        if l + 2 < L:
            pl.semaphore_wait(free, 1)
            pushes[l + 2][0].start()
            for j in range(4, 7):
                weight(l + 2, j).start()
    for i in range(NH):
        res[i] = res[i] + reduce_finish(started[i])

    gf = gf_ref[...].astype(F32)
    h = rms(jnp.concatenate([res[i] for i in range(NH)], axis=0), jnp.concatenate([gf[i:i + 1, :] for i in range(D // LANES)], axis=1))
    vocab_all(range(NCH), lambda c: c.wait())

    def tile(n, carry):
        acc = dot_t(h[:, 0:S], chunks[0][n])
        for c in range(1, NCH):
            acc = acc + dot_t(h[:, c * S:(c + 1) * S], chunks[c][n])
        acc = jnp.where(lax.broadcasted_iota(jnp.int32, (B, TN), 1) + n * TN < V, acc, -jnp.inf)
        lgt[n] = acc
        return jnp.maximum(carry, acc)

    peak = lax.fori_loop(0, NT, tile, jnp.full((B, TN), -jnp.inf, F32))
    m = jnp.max(peak, axis=-1, keepdims=True)

    def add_exp(n, carry):
        return carry + jnp.exp(lgt[n] - m)

    s = jnp.sum(lax.fori_loop(0, NT, add_exp, jnp.zeros((B, TN), F32)), axis=-1, keepdims=True)
    stat[me, 0] = jnp.broadcast_to(m, (B, LANES))
    stat[me, 1] = jnp.broadcast_to(s, (B, LANES))
    copies = [pltpu.make_async_remote_copy(src_ref=stat.at[me], dst_ref=stat.at[me], send_sem=ssend.at[k - 1], recv_sem=srecv.at[k - 1],
                                           device_id={"model": lax.rem(me + k, NM)}, device_id_type=MESH) for k in range(1, NM)]
    for c in copies:
        c.start()
    sends += copies
    score_copy.wait_recv()
    sub = lax.broadcasted_iota(jnp.int32, (B, LANES), 0)
    want = jnp.zeros((B, LANES), jnp.int32)
    for b in range(B):
        want = jnp.where(sub == b, rows[b], want)
    lane = lax.broadcasted_iota(jnp.int32, (B, LANES), 1)
    mine = jnp.where(lane + spos * B == want, scb[0, 0:1, :], 0.0)
    theirs = jnp.where(lane + (SPAN - 1 - spos) * B == want, scb[1, 0:1, :], 0.0)
    parent_score = jnp.sum(jnp.where(lane < B, mine + theirs, 0.0), axis=-1, keepdims=True)
    for c in copies:
        c.wait_recv()
    gm = stat[0, 0]
    for k in range(1, NM):
        gm = jnp.maximum(gm, stat[k, 0])
    gs = stat[0, 1] * jnp.exp(stat[0, 0] - gm)
    for k in range(1, NM):
        gs = gs + stat[k, 1] * jnp.exp(stat[k, 0] - gm)
    gm = gm[:, 0:1]
    log_s = jnp.log(gs)[:, 0:1]
    for n in range(NT):
        hi = min((n + 1) * TN, V)
        cand_ref[:, n * TN:hi] = parent_score + ((lgt[n] - gm) - log_s)[:, :hi - n * TN]
    for c in sends:
        c.wait_send()


def write_kernel(*refs):
    n = (len(refs) - 1) // 2
    sem = refs[-1]
    copies = []
    for i in range(n):
        src, dst = refs[i], refs[n + i]
        if len(src.shape) > 2:
            copies += [(src.at[j, k], dst.at[j, k]) for j in range(src.shape[0]) for k in range(src.shape[1])]
        else:
            copies.append((src, dst))
    copies = [pltpu.make_async_copy(a, b, sem.at[j]) for j, (a, b) in enumerate(copies)]
    for c in copies:
        c.start()
    for c in copies:
        c.wait()


def solution(mesh):
    data_beam = ('data', 'beam')
    cache_spec = P(None, data_beam, None, 'model', None)
    col_spec = P(None, None, 'model')
    row_spec = P(None, 'model', None)
    in_specs = (P(data_beam, None), P('data', None), P(), P(data_beam), cache_spec, cache_spec,
                P(), col_spec, col_spec, col_spec, row_spec, P(), col_spec, col_spec, row_spec, P(), P(None, 'model'))
    out_specs = (cache_spec, cache_spec, P(data_beam, 'model'))
    n_model = mesh.shape['model']

    def local_step(x_embed, parent, position, score, k_cache, v_cache, gain_attn, w_query, w_key, w_value, w_out, gain_mlp,
                   w_gate, w_up, w_down, gain_final, w_vocab):
        L, B, S, KH, HD = k_cache.shape
        D = x_embed.shape[1]
        C = KH * HD
        FF = w_gate.shape[2]
        V = w_vocab.shape[1]
        span = parent.shape[1] // B
        half = HD // 2
        freq = np.power(ROPE_BASE, -(np.arange(half, dtype=np.float64) / half)).astype(np.float32)
        freq = jnp.asarray(np.tile(freq, 2 * KH)[None])
        flat = lambda c: jnp.transpose(c, (0, 1, 3, 4, 2)).reshape(L, B, C, S)
        cfg = (L, B, D, HD, S, KH, FF, V, n_model, span)
        any_spec = pl.BlockSpec(memory_space=pl.ANY)
        vm = pl.BlockSpec(memory_space=pltpu.VMEM)
        sm = pl.BlockSpec(memory_space=pltpu.SMEM)
        steps = 2 * L
        NH = 4
        HB = B // NH
        TN = C
        NT = -(-V // TN)
        dma = pltpu.SemaphoreType.DMA
        cache_shape = (L, B, C, S)
        scratch = ([pltpu.VMEM((span * B, C, S), BF16) for _ in range(4)]
                   + [pltpu.VMEM((2, D, C), BF16)] * 3 + [pltpu.VMEM((2, C, D), BF16)]
                   + [pltpu.VMEM((2, D, FF), BF16)] * 2 + [pltpu.VMEM((2, FF, D), BF16)]
                   + [pltpu.VMEM((steps * NH * n_model, HB, D), F32), pltpu.VMEM((n_model, 2, B, LANES), F32), pltpu.VMEM((2, SUB, LANES), F32),
                      pltpu.VMEM((NH, HB, D), F32), pltpu.VMEM((NH, HB, C), F32), pltpu.VMEM((NH, HB * SUB, S), F32),
                      pltpu.VMEM((NH, HB * SUB, S), F32), pltpu.VMEM((NH, HB, C), F32), pltpu.VMEM((NT, B, TN), F32),
                      dma((2 * L,)), dma((14,)), dma((D // S * NT,)), pltpu.SemaphoreType.REGULAR, dma((2 * L,)), dma((2 * L,)),
                      dma((steps * NH * (n_model - 1),)), dma((steps * NH * n_model,)), dma((n_model - 1,)), dma((n_model - 1,)),
                      dma, dma])
        limit = 64 * 1024 * 1024 - 65536
        outs = pl.pallas_call(
            functools.partial(decode_kernel, cfg),
            out_shape=(pltpu.VMEM(cache_shape, BF16), pltpu.VMEM(cache_shape, BF16), pltpu.VMEM((B, V), F32)),
            in_specs=[sm, sm, vm, vm, vm, vm, vm, vm] + [any_spec] * 10,
            out_specs=(vm, vm, vm),
            scratch_shapes=scratch,
            compiler_params=pltpu.CompilerParams(collective_id=0, has_side_effects=True,
                                                 vmem_limit_bytes=limit - 2 * L * B * C * S * 2 - B * (V + LANES) * 4 - (1 << 19)),
            name="decode_step",
        )(parent, position.reshape(1), x_embed, score[None], freq, gain_attn, gain_mlp, gain_final.reshape(D // LANES, LANES),
          flat(k_cache), flat(v_cache), w_query, w_key, w_value, w_out, w_gate, w_up, w_down, w_vocab.T)
        k_out, v_out, cand = pl.pallas_call(
            write_kernel,
            out_shape=(jax.ShapeDtypeStruct(cache_shape, BF16), jax.ShapeDtypeStruct(cache_shape, BF16),
                       jax.ShapeDtypeStruct((B, V), F32)),
            in_specs=[vm, vm, vm],
            out_specs=(any_spec, any_spec, any_spec),
            scratch_shapes=[dma((2 * L * B + 1,))],
            compiler_params=pltpu.CompilerParams(vmem_limit_bytes=1 << 20),
            name="write_out",
        )(*outs)
        back = lambda c: jnp.transpose(c.reshape(L, B, KH, HD, S), (0, 1, 4, 2, 3))
        return back(k_out), back(v_out), cand

    return jax.shard_map(local_step, mesh=mesh, in_specs=in_specs, out_specs=out_specs, check_vma=False)
```

```python
import functools

import jax
import jax.numpy as jnp
import numpy as np
from jax import lax
from jax.experimental import pallas as pl
from jax.experimental.pallas import tpu as pltpu
from jax.sharding import PartitionSpec as P

NORM_EPS = 1e-6
ROPE_BASE = 10000.0
MESH = pl.DeviceIdType.MESH
F32 = jnp.float32
BF16 = jnp.bfloat16
LANES = 128
SUB = 8


def rms(res, gain):
    inv = lax.rsqrt(jnp.mean(res * res, axis=-1, keepdims=True) + NORM_EPS)
    return (res * inv * gain.astype(F32)).astype(BF16)


def dot(a, b):
    return jnp.dot(a, b, preferred_element_type=F32)


def dot_t(a, b):
    return lax.dot_general(a, b, (((1,), (1,)), ((), ())), preferred_element_type=F32)


def decode_kernel(cfg, *refs):
    L, B, D, HD, S, KH, FF, V, NM, SPAN = cfg
    (parent_ref, pos_ref, x_ref, score_ref, freq_ref, ga_ref, gm_ref, gf_ref,
     kc, vc, wq, wk, wv, wo, wg, wu, wd, wt, kst, vst, cand_ref,
     kb0, kb1, kb2, vb0, vb1, vb2, wqb, wkb, wvb, wob, wgb, wub, wdb, ar, stat, scb, xb, kn, vn, res, qs, lg, pr, osc, osend, orecv, lgt,
     sem_c, sem_w, sem_t, free, bsend, brecv, asend, arecv, ssend, srecv, csend, crecv, xsend, xrecv, hsend, hrecv) = refs
    slots = [0] + [1 + (l + 1) % 2 for l in range(1, L)]
    kb = [(kb0, kb1, kb2)[j] for j in slots]
    vb = [(vb0, vb1, vb2)[j] for j in slots]
    C = KH * HD
    NH, HB = res.shape[:2]
    me = lax.axis_index("model")
    beam = lax.axis_index("beam")
    spos = lax.rem(beam, SPAN)
    sent = lax.div(beam, SPAN)
    partner = beam - spos + lax.rem(spos + 1, SPAN)
    own = pl.ds(spos * B, B)

    def cache_local(l):
        return (pltpu.make_async_copy(kc.at[l], kb[l].at[own], sem_c.at[2 * l]),
                pltpu.make_async_copy(vc.at[l], vb[l].at[own], sem_c.at[2 * l + 1]))

    def cache_push(l):
        return tuple(pltpu.make_async_remote_copy(src_ref=c.at[l], dst_ref=buf[l].at[own], send_sem=bsend.at[2 * l + i],
                                                  recv_sem=brecv.at[2 * l + i], device_id={"beam": partner}, device_id_type=MESH)
                     for i, (c, buf) in enumerate(((kc, kb), (vc, vb))))

    weights = ((wq, wqb), (wk, wkb), (wv, wvb), (wo, wob), (wg, wgb), (wu, wub), (wd, wdb))

    def weight(l, i):
        src, buf = weights[i]
        return pltpu.make_async_copy(src.at[l], buf.at[l % 2], sem_w.at[(l % 2) * 7 + i])

    chunks = (kb1, vb1, kb2, vb2)
    NCH = D // S
    NT = lgt.shape[0]
    TN = lgt.shape[2]

    def vocab(c, n, rows=TN):
        start = n * TN if isinstance(n, int) else pl.multiple_of(n * TN, TN)
        return pltpu.make_async_copy(wt.at[pl.ds(start, rows), c * S:(c + 1) * S], chunks[c].at[n, pl.ds(0, rows)],
                                     sem_t.at[c * NT + n])

    def vocab_all(which, act):
        def body(n, carry):
            for c in which:
                act(vocab(c, n))
            return carry
        full = V // TN
        lax.fori_loop(0, full, body, 0)
        if full < NT:
            for c in which:
                act(vocab(c, full, V - full * TN))

    for i in range(3):
        weight(0, i).start()
    for c in cache_local(0):
        c.start()

    barrier = pltpu.get_barrier_semaphore()
    for k in range(1, NM):
        pl.semaphore_signal(barrier, inc=1, device_id={"model": lax.rem(me + k, NM)}, device_id_type=MESH)
    pl.semaphore_signal(barrier, inc=1, device_id={"beam": partner}, device_id_type=MESH)

    scb[0] = jnp.zeros((SUB, LANES), F32)
    scb[0, 0:1, 0:B] = score_ref[...]
    pos = pos_ref[0]
    angle = pos.astype(F32) * freq_ref[...]
    cos = jnp.cos(angle)
    sin = jnp.sin(angle)
    rows = [lax.rem(parent_ref[sent, spos * B + b], SPAN * B) for b in range(B)]
    near = [spos * B + lax.rem(r, B) for r in rows]
    far = [spos * B + lax.rem(parent_ref[sent, (SPAN - 1 - spos) * B + b], B) for b in range(B)]

    def rope(x):
        low = lax.rem(lax.broadcasted_iota(jnp.int32, x.shape, 1), HD) < HD // 2
        other = jnp.where(low, -pltpu.roll(x, C - HD // 2, 1), pltpu.roll(x, HD // 2, 1))
        return x * cos + other * sin

    def project(l, r):
        ws = l % 2
        h = rms(r, ga_ref[l:l + 1, :])
        q = rope(dot(h, wqb[ws])).astype(BF16).astype(F32)
        k = rope(dot(h, wkb[ws])).astype(BF16).astype(F32)
        v = dot(h, wvb[ws]).astype(BF16).astype(F32)
        return q * (HD ** -0.5), k, v

    for j in range(3):
        weight(0, j).wait()
    own_q, own_k, own_v = project(0, x_ref[...].astype(F32))
    kn[...] = own_k
    vn[...] = own_v

    pl.semaphore_wait(barrier, NM)

    pushes = [cache_push(l) for l in range(L)]
    x_copy = pltpu.make_async_remote_copy(src_ref=x_ref, dst_ref=xb, send_sem=xsend, recv_sem=xrecv,
                                          device_id={"beam": partner}, device_id_type=MESH)
    x_copy.start()
    score_copy = pltpu.make_async_remote_copy(src_ref=scb.at[0], dst_ref=scb.at[1], send_sem=csend, recv_sem=crecv,
                                              device_id={"beam": partner}, device_id_type=MESH)
    score_copy.start()
    for i in range(3, 7):
        weight(0, i).start()
    for c in cache_local(1):
        c.start()
    for i in range(7):
        weight(1, i).start()

    def peers():
        if NM == 4:
            side = lax.div(me, 2)
            return [3 - 3 * side, 2 - side, me + 1 - 2 * lax.rem(me, 2)]
        return [lax.rem(me + k, NM) for k in range(1, NM)]

    def reduce_copy(step, j, source, peer):
        slot = step * NM + source
        return pltpu.make_async_remote_copy(src_ref=ar.at[slot], dst_ref=ar.at[slot], send_sem=asend.at[step * (NM - 1) + j],
                                            recv_sem=arecv.at[slot], device_id={"model": peer}, device_id_type=MESH)

    def reduce_start(step, value):
        ar[step * NM + me] = value
        copies = [reduce_copy(step, j, me, peer) for j, peer in enumerate(peers())]
        for c in copies:
            c.start()
        sends.extend(copies)
        return step

    def reduce_finish(step):
        for k in range(1, NM):
            reduce_copy(step, 0, lax.rem(me + k, NM), me).wait_recv()
        total = ar[step * NM]
        for k in range(1, NM):
            total = total + ar[step * NM + k]
        return total

    head_of_lane = lax.broadcasted_iota(jnp.int32, (SUB, C), 1) // HD
    head_mask = head_of_lane == lax.broadcasted_iota(jnp.int32, (SUB, C), 0)
    here = lax.broadcasted_iota(jnp.int32, (C, S), 1) == pos
    sends = [score_copy, x_copy]
    sends.extend(pushes[l][i] for l in range(L) for i in range(2))

    def columns(x):
        return jnp.concatenate([x, jnp.zeros((LANES - x.shape[0], C), F32)], axis=0).T

    def insert(cols, b, row):
        return jnp.where(here, jnp.broadcast_to(cols[:, b:b + 1], (C, S)).astype(BF16), row)

    def attention(l, i, q, k, v, index, out, keep, ready):
        qs[i] = q
        k_cols = columns(k)
        v_cols = columns(v)
        ready(0)
        for b in range(HB):
            kept = insert(k_cols, b, kb[l][index[i * HB + b]])
            if keep:
                kst[l, i * HB + b] = kept
            qb = jnp.where(head_mask, jnp.broadcast_to(qs[i, b:b + 1, :], (SUB, C)), 0.0).astype(BF16)
            lg[i, b * SUB:(b + 1) * SUB, :] = dot(qb, kept)
        logits = lg[i]
        logits = jnp.where(lax.broadcasted_iota(jnp.int32, logits.shape, 1) <= pos, logits, -jnp.inf)
        e = jnp.exp(logits - jnp.max(logits, axis=-1, keepdims=True))
        pr[i] = e / jnp.sum(e, axis=-1, keepdims=True)
        ready(1)
        for b in range(HB):
            kept = insert(v_cols, b, vb[l][index[i * HB + b]])
            if keep:
                vst[l, i * HB + b] = kept
            ob = dot_t(pr[i, b * SUB:(b + 1) * SUB, :].astype(BF16), kept)
            out[i, b:b + 1, :] = jnp.sum(jnp.where(head_mask, ob, 0.0), axis=0, keepdims=True)

    def project_out(l, i, o):
        if i == 0:
            weight(l, 3).wait()
        return reduce_start(2 * l * NH + i, dot(o.astype(BF16), wob[l % 2]))

    def attend(l, i, r):
        if i == 0:
            for j in range(3):
                weight(l, j).wait()
        q, k, v = project(l, r)

        def ready(which):
            if i == 0:
                cache_local(l)[which].wait()
                pushes[l][which].wait_recv()

        attention(l, i, q, k, v, rows, osc, True, ready)
        return project_out(l, i, osc[i])

    def attend_first():
        for c in cache_local(0):
            c.wait()
        part = lambda x, i: x[i * HB:(i + 1) * HB, :]
        for i in range(NH):
            attention(0, i, part(own_q, i), part(own_k, i), part(own_v, i), near, osc, False, lambda w: None)
        x_copy.wait_recv()
        q, k, v = project(0, xb[...].astype(F32))
        copies = []
        for i in range(NH):
            attention(0, i, part(q, i), part(k, i), part(v, i), far, osend, False, lambda w: None)
            copies.append(pltpu.make_async_remote_copy(src_ref=osend.at[i], dst_ref=orecv.at[i], send_sem=hsend.at[i], recv_sem=hrecv.at[i],
                                                       device_id={"beam": partner}, device_id_type=MESH))
            copies[i].start()
        sends.extend(copies)
        steps = []
        for i in range(NH):
            copies[i].wait_recv()
            home = jnp.zeros((HB, C), jnp.int32)
            for b in range(HB):
                home = jnp.where(lax.broadcasted_iota(jnp.int32, (HB, C), 0) == b, lax.div(rows[i * HB + b], B), home)
            steps.append(project_out(0, i, jnp.where(home == spos, osc[i], orecv[i])))
        return steps

    def keep_first(which):
        cols = columns((kn, vn)[which][...])
        pushes[0][which].wait_recv()
        for b in range(B):
            (kst, vst)[which][0, b] = insert(cols, b, (kb, vb)[which][0][rows[b]])

    def mlp(l, i, r):
        ws = l % 2
        h = rms(r, gm_ref[l:l + 1, :])
        if i == 0:
            weight(l, 4).wait()
            weight(l, 5).wait()
        gate = dot(h, wgb[ws])
        up = dot(h, wub[ws])
        g = (gate * jax.nn.sigmoid(gate) * up).astype(BF16)
        if i == 0:
            weight(l, 6).wait()
        return reduce_start((2 * l + 1) * NH + i, dot(g, wdb[ws]))

    for i in range(NH):
        res[i] = x_ref[i * HB:(i + 1) * HB, :].astype(F32)
    started = attend_first()
    order = [(1, 0), (1, 1)] + [(l, w) for l in range(2, L) for w in range(2)] + [(0, 0), (0, 1)]
    order = [order[:2]] + [[o] for o in order[2:]]
    for l in range(L):
        if l > 0:
            for i in range(NH):
                res[i] = res[i] + reduce_finish(started[i])
                started[i] = attend(l, i, res[i])
            if l + 2 < L:
                pl.semaphore_signal(free, inc=1, device_id={"beam": partner}, device_id_type=MESH)
        for o in order[2 * l] if 2 * l < len(order) else []:
            pushes[o[0]][o[1]].start()
        if l + 2 < L:
            for c in cache_local(l + 2):
                c.start()
            for j in range(4):
                weight(l + 2, j).start()
        if l == L - 1:
            vocab_all(range(NCH), lambda c: c.start())
            keep_first(0)
        for i in range(NH):
            res[i] = res[i] + reduce_finish(started[i])
            started[i] = mlp(l, i, res[i])
        for o in order[2 * l + 1] if 2 * l + 1 < len(order) else []:
            if o[0] >= 3 and o[1] == 0:
                pl.semaphore_wait(free, 1)
            pushes[o[0]][o[1]].start()
        if l + 2 < L:
            for j in range(4, 7):
                weight(l + 2, j).start()
        if l == L - 1:
            keep_first(1)
    for i in range(NH):
        res[i] = res[i] + reduce_finish(started[i])

    gf = gf_ref[...].astype(F32)
    h = rms(jnp.concatenate([res[i] for i in range(NH)], axis=0), jnp.concatenate([gf[i:i + 1, :] for i in range(D // LANES)], axis=1))
    vocab_all(range(NCH), lambda c: c.wait())

    def tile(n, carry):
        acc = dot_t(h[:, 0:S], chunks[0][n])
        for c in range(1, NCH):
            acc = acc + dot_t(h[:, c * S:(c + 1) * S], chunks[c][n])
        acc = jnp.where(lax.broadcasted_iota(jnp.int32, (B, TN), 1) + n * TN < V, acc, -jnp.inf)
        lgt[n] = acc
        return jnp.maximum(carry, acc)

    peak = lax.fori_loop(0, NT, tile, jnp.full((B, TN), -jnp.inf, F32))
    m = jnp.max(peak, axis=-1, keepdims=True)

    def add_exp(n, carry):
        return carry + jnp.exp(lgt[n] - m)

    s = jnp.sum(lax.fori_loop(0, NT, add_exp, jnp.zeros((B, TN), F32)), axis=-1, keepdims=True)
    stat[me, 0] = jnp.broadcast_to(m, (B, LANES))
    stat[me, 1] = jnp.broadcast_to(s, (B, LANES))
    copies = [pltpu.make_async_remote_copy(src_ref=stat.at[me], dst_ref=stat.at[me], send_sem=ssend.at[k - 1], recv_sem=srecv.at[k - 1],
                                           device_id={"model": lax.rem(me + k, NM)}, device_id_type=MESH) for k in range(1, NM)]
    for c in copies:
        c.start()
    sends += copies
    score_copy.wait_recv()
    sub = lax.broadcasted_iota(jnp.int32, (B, LANES), 0)
    want = jnp.zeros((B, LANES), jnp.int32)
    for b in range(B):
        want = jnp.where(sub == b, rows[b], want)
    lane = lax.broadcasted_iota(jnp.int32, (B, LANES), 1)
    mine = jnp.where(lane + spos * B == want, scb[0, 0:1, :], 0.0)
    theirs = jnp.where(lane + (SPAN - 1 - spos) * B == want, scb[1, 0:1, :], 0.0)
    parent_score = jnp.sum(jnp.where(lane < B, mine + theirs, 0.0), axis=-1, keepdims=True)
    for c in copies:
        c.wait_recv()
    gm = stat[0, 0]
    for k in range(1, NM):
        gm = jnp.maximum(gm, stat[k, 0])
    gs = stat[0, 1] * jnp.exp(stat[0, 0] - gm)
    for k in range(1, NM):
        gs = gs + stat[k, 1] * jnp.exp(stat[k, 0] - gm)
    gm = gm[:, 0:1]
    log_s = jnp.log(gs)[:, 0:1]
    for n in range(NT):
        hi = min((n + 1) * TN, V)
        cand_ref[:, n * TN:hi] = parent_score + ((lgt[n] - gm) - log_s)[:, :hi - n * TN]
    for c in sends:
        c.wait_send()


def write_kernel(*refs):
    n = (len(refs) - 1) // 2
    sem = refs[-1]
    copies = []
    for i in range(n):
        src, dst = refs[i], refs[n + i]
        if len(src.shape) > 2:
            copies += [(src.at[j], dst.at[j]) for j in range(src.shape[0])]
        else:
            copies.append((src, dst))
    copies = [pltpu.make_async_copy(a, b, sem.at[j]) for j, (a, b) in enumerate(copies)]
    for c in copies:
        c.start()
    for c in copies:
        c.wait()


def solution(mesh):
    data_beam = ('data', 'beam')
    cache_spec = P(None, data_beam, None, 'model', None)
    col_spec = P(None, None, 'model')
    row_spec = P(None, 'model', None)
    in_specs = (P(data_beam, None), P('data', None), P(), P(data_beam), cache_spec, cache_spec,
                P(), col_spec, col_spec, col_spec, row_spec, P(), col_spec, col_spec, row_spec, P(), P(None, 'model'))
    out_specs = (cache_spec, cache_spec, P(data_beam, 'model'))
    n_model = mesh.shape['model']

    def local_step(x_embed, parent, position, score, k_cache, v_cache, gain_attn, w_query, w_key, w_value, w_out, gain_mlp,
                   w_gate, w_up, w_down, gain_final, w_vocab):
        L, B, S, KH, HD = k_cache.shape
        D = x_embed.shape[1]
        C = KH * HD
        FF = w_gate.shape[2]
        V = w_vocab.shape[1]
        span = parent.shape[1] // B
        half = HD // 2
        freq = np.power(ROPE_BASE, -(np.arange(half, dtype=np.float64) / half)).astype(np.float32)
        freq = jnp.asarray(np.tile(freq, 2 * KH)[None])
        flat = lambda c: jnp.transpose(c, (0, 1, 3, 4, 2)).reshape(L, B, C, S)
        cfg = (L, B, D, HD, S, KH, FF, V, n_model, span)
        any_spec = pl.BlockSpec(memory_space=pl.ANY)
        vm = pl.BlockSpec(memory_space=pltpu.VMEM)
        sm = pl.BlockSpec(memory_space=pltpu.SMEM)
        steps = 2 * L
        NH = 4
        HB = B // NH
        TN = C
        NT = -(-V // TN)
        dma = pltpu.SemaphoreType.DMA
        cache_shape = (L, B, C, S)
        scratch = ([pltpu.VMEM((span * B, C, S), BF16) for _ in range(6)]
                   + [pltpu.VMEM((2, D, C), BF16)] * 3 + [pltpu.VMEM((2, C, D), BF16)]
                   + [pltpu.VMEM((2, D, FF), BF16)] * 2 + [pltpu.VMEM((2, FF, D), BF16)]
                   + [pltpu.VMEM((steps * NH * n_model, HB, D), F32), pltpu.VMEM((n_model, 2, B, LANES), F32), pltpu.VMEM((2, SUB, LANES), F32),
                      pltpu.VMEM((B, D), BF16), pltpu.VMEM((B, C), F32), pltpu.VMEM((B, C), F32),
                      pltpu.VMEM((NH, HB, D), F32), pltpu.VMEM((NH, HB, C), F32), pltpu.VMEM((NH, HB * SUB, S), F32),
                      pltpu.VMEM((NH, HB * SUB, S), F32)] + [pltpu.VMEM((NH, HB, C), F32)] * 3 + [ pltpu.VMEM((NT, B, TN), F32),
                      dma((2 * L,)), dma((14,)), dma((D // S * NT,)), pltpu.SemaphoreType.REGULAR, dma((2 * L,)), dma((2 * L,)),
                      dma((steps * NH * (n_model - 1),)), dma((steps * NH * n_model,)), dma((n_model - 1,)), dma((n_model - 1,)),
                      dma, dma, dma, dma, dma((NH,)), dma((NH,))])
        limit = 64 * 1024 * 1024 - 65536
        outs = pl.pallas_call(
            functools.partial(decode_kernel, cfg),
            out_shape=(pltpu.VMEM(cache_shape, BF16), pltpu.VMEM(cache_shape, BF16), pltpu.VMEM((B, V), F32)),
            in_specs=[sm, sm, vm, vm, vm, vm, vm, vm] + [any_spec] * 10,
            out_specs=(vm, vm, vm),
            scratch_shapes=scratch,
            compiler_params=pltpu.CompilerParams(collective_id=0, has_side_effects=True,
                                                 vmem_limit_bytes=limit - 2 * L * B * C * S * 2 - B * (V + LANES) * 4 - (1 << 19)),
            name="decode_step",
        )(parent, position.reshape(1), x_embed, score[None], freq, gain_attn, gain_mlp, gain_final.reshape(D // LANES, LANES),
          flat(k_cache), flat(v_cache), w_query, w_key, w_value, w_out, w_gate, w_up, w_down, w_vocab.T)
        k_out, v_out, cand = pl.pallas_call(
            write_kernel,
            out_shape=(jax.ShapeDtypeStruct(cache_shape, BF16), jax.ShapeDtypeStruct(cache_shape, BF16),
                       jax.ShapeDtypeStruct((B, V), F32)),
            in_specs=[vm, vm, vm],
            out_specs=(any_spec, any_spec, any_spec),
            scratch_shapes=[dma((2 * L + 1,))],
            compiler_params=pltpu.CompilerParams(vmem_limit_bytes=1 << 20),
            name="write_out",
        )(*outs)
        back = lambda c: jnp.transpose(c.reshape(L, B, KH, HD, S), (0, 1, 4, 2, 3))
        return back(k_out), back(v_out), cand

    return jax.shard_map(local_step, mesh=mesh, in_specs=in_specs, out_specs=out_specs, check_vma=False)
```

```python
import functools

import jax
import jax.numpy as jnp
import numpy as np
from jax import lax
from jax.experimental import pallas as pl
from jax.experimental.pallas import tpu as pltpu
from jax.sharding import PartitionSpec as P

NORM_EPS = 1e-6
ROPE_BASE = 10000.0
MESH = pl.DeviceIdType.MESH
F32 = jnp.float32
BF16 = jnp.bfloat16
LANES = 128
SUB = 8


def rms(res, gain):
    inv = lax.rsqrt(jnp.mean(res * res, axis=-1, keepdims=True) + NORM_EPS)
    return (res * inv * gain.astype(F32)).astype(BF16)


def dot(a, b):
    return jnp.dot(a, b, preferred_element_type=F32)


def dot_t(a, b):
    return lax.dot_general(a, b, (((1,), (1,)), ((), ())), preferred_element_type=F32)


def decode_kernel(cfg, *refs):
    L, B, D, HD, S, KH, FF, V, NM, SPAN = cfg
    (parent_ref, pos_ref, x_ref, score_ref, freq_ref, ga_ref, gm_ref, gf_ref,
     kc, vc, wq, wk, wv, wo, wg, wu, wd, wt, kst, vst, cand_ref,
     kb0, kb1, kb2, vb0, vb1, vb2, wqb, wkb, wvb, wob, wgb, wub, wdb, ar, stat, scb, xb, kn, vn, res, qs, lg, pr, osc, osend, orecv, lgt,
     sem_c, sem_w, sem_t, free, bsend, brecv, asend, arecv, ssend, srecv, csend, crecv, xsend, xrecv, hsend, hrecv) = refs
    slots = [0] + [1 + (l + 1) % 2 for l in range(1, L)]
    kb = [(kb0, kb1, kb2)[j] for j in slots]
    vb = [(vb0, vb1, vb2)[j] for j in slots]
    C = KH * HD
    NH, HB = res.shape[:2]
    me = lax.axis_index("model")
    beam = lax.axis_index("beam")
    spos = lax.rem(beam, SPAN)
    sent = lax.div(beam, SPAN)
    partner = beam - spos + lax.rem(spos + 1, SPAN)
    own = pl.ds(spos * B, B)

    def cache_local(l):
        return (pltpu.make_async_copy(kc.at[l], kb[l].at[own], sem_c.at[2 * l]),
                pltpu.make_async_copy(vc.at[l], vb[l].at[own], sem_c.at[2 * l + 1]))

    def cache_push(l):
        return tuple(pltpu.make_async_remote_copy(src_ref=buf[l].at[own], dst_ref=buf[l].at[own], send_sem=bsend.at[2 * l + i],
                                                  recv_sem=brecv.at[2 * l + i], device_id={"beam": partner}, device_id_type=MESH)
                     for i, buf in enumerate((kb, vb)))

    weights = ((wq, wqb), (wk, wkb), (wv, wvb), (wo, wob), (wg, wgb), (wu, wub), (wd, wdb))

    def weight(l, i):
        src, buf = weights[i]
        return pltpu.make_async_copy(src.at[l], buf.at[l % 2], sem_w.at[(l % 2) * 7 + i])

    chunks = (kb1, vb1, kb2, vb2)
    NCH = D // S
    NT = lgt.shape[0]
    TN = lgt.shape[2]

    def vocab(c, n, rows=TN):
        start = n * TN if isinstance(n, int) else pl.multiple_of(n * TN, TN)
        return pltpu.make_async_copy(wt.at[pl.ds(start, rows), c * S:(c + 1) * S], chunks[c].at[n, pl.ds(0, rows)],
                                     sem_t.at[c * NT + n])

    def vocab_all(which, act):
        def body(n, carry):
            for c in which:
                act(vocab(c, n))
            return carry
        full = V // TN
        lax.fori_loop(0, full, body, 0)
        if full < NT:
            for c in which:
                act(vocab(c, full, V - full * TN))

    for i in range(3):
        weight(0, i).start()
    for c in cache_local(0):
        c.start()

    barrier = pltpu.get_barrier_semaphore()
    for k in range(1, NM):
        pl.semaphore_signal(barrier, inc=1, device_id={"model": lax.rem(me + k, NM)}, device_id_type=MESH)
    pl.semaphore_signal(barrier, inc=1, device_id={"beam": partner}, device_id_type=MESH)

    scb[0] = jnp.zeros((SUB, LANES), F32)
    scb[0, 0:1, 0:B] = score_ref[...]
    pos = pos_ref[0]
    angle = pos.astype(F32) * freq_ref[...]
    cos = jnp.cos(angle)
    sin = jnp.sin(angle)
    rows = [lax.rem(parent_ref[sent, spos * B + b], SPAN * B) for b in range(B)]
    near = [spos * B + lax.rem(r, B) for r in rows]
    far = [spos * B + lax.rem(parent_ref[sent, (SPAN - 1 - spos) * B + b], B) for b in range(B)]

    def rope(x):
        low = lax.rem(lax.broadcasted_iota(jnp.int32, x.shape, 1), HD) < HD // 2
        other = jnp.where(low, -pltpu.roll(x, C - HD // 2, 1), pltpu.roll(x, HD // 2, 1))
        return x * cos + other * sin

    def project(l, r):
        ws = l % 2
        h = rms(r, ga_ref[l:l + 1, :])
        q = rope(dot(h, wqb[ws])).astype(BF16).astype(F32)
        k = rope(dot(h, wkb[ws])).astype(BF16).astype(F32)
        v = dot(h, wvb[ws]).astype(BF16).astype(F32)
        return q * (HD ** -0.5), k, v

    for j in range(3):
        weight(0, j).wait()
    own_q, own_k, own_v = project(0, x_ref[...].astype(F32))
    kn[...] = own_k
    vn[...] = own_v

    pl.semaphore_wait(barrier, NM)

    pushes = [cache_push(l) for l in range(L)]
    x_copy = pltpu.make_async_remote_copy(src_ref=x_ref, dst_ref=xb, send_sem=xsend, recv_sem=xrecv,
                                          device_id={"beam": partner}, device_id_type=MESH)
    x_copy.start()
    score_copy = pltpu.make_async_remote_copy(src_ref=scb.at[0], dst_ref=scb.at[1], send_sem=csend, recv_sem=crecv,
                                              device_id={"beam": partner}, device_id_type=MESH)
    score_copy.start()
    for i in range(3, 7):
        weight(0, i).start()
    for c in cache_local(1):
        c.start()
    for i in range(7):
        weight(1, i).start()

    def peers():
        if NM == 4:
            side = lax.div(me, 2)
            return [3 - 3 * side, 2 - side, me + 1 - 2 * lax.rem(me, 2)]
        return [lax.rem(me + k, NM) for k in range(1, NM)]

    def reduce_copy(step, j, source, peer):
        slot = step * NM + source
        return pltpu.make_async_remote_copy(src_ref=ar.at[slot], dst_ref=ar.at[slot], send_sem=asend.at[step * (NM - 1) + j],
                                            recv_sem=arecv.at[slot], device_id={"model": peer}, device_id_type=MESH)

    def reduce_start(step, value):
        ar[step * NM + me] = value
        copies = [reduce_copy(step, j, me, peer) for j, peer in enumerate(peers())]
        for c in copies:
            c.start()
        sends.extend(copies)
        return step

    def reduce_finish(step):
        for k in range(1, NM):
            reduce_copy(step, 0, lax.rem(me + k, NM), me).wait_recv()
        total = ar[step * NM]
        for k in range(1, NM):
            total = total + ar[step * NM + k]
        return total

    head_of_lane = lax.broadcasted_iota(jnp.int32, (SUB, C), 1) // HD
    head_mask = head_of_lane == lax.broadcasted_iota(jnp.int32, (SUB, C), 0)
    here = lax.broadcasted_iota(jnp.int32, (C, S), 1) == pos
    sends = [score_copy, x_copy]

    def columns(x):
        return jnp.concatenate([x, jnp.zeros((LANES - x.shape[0], C), F32)], axis=0).T

    def insert(cols, b, row):
        return jnp.where(here, jnp.broadcast_to(cols[:, b:b + 1], (C, S)).astype(BF16), row)

    def attention(l, i, q, k, v, index, out, keep, ready):
        qs[i] = q
        k_cols = columns(k)
        v_cols = columns(v)
        ready(0)
        for b in range(HB):
            kept = insert(k_cols, b, kb[l][index[i * HB + b]])
            if keep:
                kst[l, i * HB + b] = kept
            qb = jnp.where(head_mask, jnp.broadcast_to(qs[i, b:b + 1, :], (SUB, C)), 0.0).astype(BF16)
            lg[i, b * SUB:(b + 1) * SUB, :] = dot(qb, kept)
        logits = lg[i]
        logits = jnp.where(lax.broadcasted_iota(jnp.int32, logits.shape, 1) <= pos, logits, -jnp.inf)
        e = jnp.exp(logits - jnp.max(logits, axis=-1, keepdims=True))
        pr[i] = e / jnp.sum(e, axis=-1, keepdims=True)
        ready(1)
        for b in range(HB):
            kept = insert(v_cols, b, vb[l][index[i * HB + b]])
            if keep:
                vst[l, i * HB + b] = kept
            ob = dot_t(pr[i, b * SUB:(b + 1) * SUB, :].astype(BF16), kept)
            out[i, b:b + 1, :] = jnp.sum(jnp.where(head_mask, ob, 0.0), axis=0, keepdims=True)

    def project_out(l, i, o):
        if i == 0:
            weight(l, 3).wait()
        return reduce_start(2 * l * NH + i, dot(o.astype(BF16), wob[l % 2]))

    def attend(l, i, r):
        if i == 0:
            for j in range(3):
                weight(l, j).wait()
        q, k, v = project(l, r)

        def ready(which):
            if i == 0:
                pushes[l][which].wait_recv()

        attention(l, i, q, k, v, rows, osc, True, ready)
        return project_out(l, i, osc[i])

    def attend_first():
        for c in cache_local(0):
            c.wait()
        part = lambda x, i: x[i * HB:(i + 1) * HB, :]
        for i in range(NH):
            attention(0, i, part(own_q, i), part(own_k, i), part(own_v, i), near, osc, False, lambda w: None)
        x_copy.wait_recv()
        q, k, v = project(0, xb[...].astype(F32))
        copies = []
        for i in range(NH):
            attention(0, i, part(q, i), part(k, i), part(v, i), far, osend, False, lambda w: None)
            copies.append(pltpu.make_async_remote_copy(src_ref=osend.at[i], dst_ref=orecv.at[i], send_sem=hsend.at[i], recv_sem=hrecv.at[i],
                                                       device_id={"beam": partner}, device_id_type=MESH))
            copies[i].start()
        sends.extend(copies)
        steps = []
        for i in range(NH):
            copies[i].wait_recv()
            home = jnp.zeros((HB, C), jnp.int32)
            for b in range(HB):
                home = jnp.where(lax.broadcasted_iota(jnp.int32, (HB, C), 0) == b, lax.div(rows[i * HB + b], B), home)
            steps.append(project_out(0, i, jnp.where(home == spos, osc[i], orecv[i])))
        return steps

    def keep_first(which):
        cols = columns((kn, vn)[which][...])
        pushes[0][which].wait_recv()
        for b in range(B):
            (kst, vst)[which][0, b] = insert(cols, b, (kb, vb)[which][0][rows[b]])

    def mlp(l, i, r):
        ws = l % 2
        h = rms(r, gm_ref[l:l + 1, :])
        if i == 0:
            weight(l, 4).wait()
            weight(l, 5).wait()
        gate = dot(h, wgb[ws])
        up = dot(h, wub[ws])
        g = (gate * jax.nn.sigmoid(gate) * up).astype(BF16)
        if i == 0:
            weight(l, 6).wait()
        return reduce_start((2 * l + 1) * NH + i, dot(g, wdb[ws]))

    for i in range(NH):
        res[i] = x_ref[i * HB:(i + 1) * HB, :].astype(F32)
    def push(l, which):
        if l > 0:
            cache_local(l)[which].wait()
        pushes[l][which].start()

    started = attend_first()
    order = [(1, 0), (1, 1)] + [(l, w) for l in range(2, L) for w in range(2)] + [(0, 0), (0, 1)]
    order = [order[:2]] + [[o] for o in order[2:]]
    for l in range(L):
        if l > 0:
            for i in range(NH):
                res[i] = res[i] + reduce_finish(started[i])
                started[i] = attend(l, i, res[i])
            if l + 2 < L:
                pl.semaphore_signal(free, inc=1, device_id={"beam": partner}, device_id_type=MESH)
        for o in order[2 * l] if 2 * l < len(order) else []:
            push(*o)
        if l + 2 < L:
            for which in range(2):
                if l > 0:
                    pushes[l][which].wait_send()
                cache_local(l + 2)[which].start()
            for j in range(4):
                weight(l + 2, j).start()
        if l == L - 1:
            for j in (l - 1, l):
                for which in range(2):
                    pushes[j][which].wait_send()
            vocab_all(range(NCH), lambda c: c.start())
            keep_first(0)
        for i in range(NH):
            res[i] = res[i] + reduce_finish(started[i])
            started[i] = mlp(l, i, res[i])
        for o in order[2 * l + 1] if 2 * l + 1 < len(order) else []:
            if o[0] >= 3 and o[1] == 0:
                pl.semaphore_wait(free, 1)
            push(*o)
        if l + 2 < L:
            for j in range(4, 7):
                weight(l + 2, j).start()
        if l == L - 1:
            keep_first(1)
    for i in range(NH):
        res[i] = res[i] + reduce_finish(started[i])

    gf = gf_ref[...].astype(F32)
    h = rms(jnp.concatenate([res[i] for i in range(NH)], axis=0), jnp.concatenate([gf[i:i + 1, :] for i in range(D // LANES)], axis=1))
    vocab_all(range(NCH), lambda c: c.wait())

    def tile(n, carry):
        acc = dot_t(h[:, 0:S], chunks[0][n])
        for c in range(1, NCH):
            acc = acc + dot_t(h[:, c * S:(c + 1) * S], chunks[c][n])
        acc = jnp.where(lax.broadcasted_iota(jnp.int32, (B, TN), 1) + n * TN < V, acc, -jnp.inf)
        lgt[n] = acc
        return jnp.maximum(carry, acc)

    peak = lax.fori_loop(0, NT, tile, jnp.full((B, TN), -jnp.inf, F32))
    m = jnp.max(peak, axis=-1, keepdims=True)

    def add_exp(n, carry):
        return carry + jnp.exp(lgt[n] - m)

    s = jnp.sum(lax.fori_loop(0, NT, add_exp, jnp.zeros((B, TN), F32)), axis=-1, keepdims=True)
    stat[me, 0] = jnp.broadcast_to(m, (B, LANES))
    stat[me, 1] = jnp.broadcast_to(s, (B, LANES))
    copies = [pltpu.make_async_remote_copy(src_ref=stat.at[me], dst_ref=stat.at[me], send_sem=ssend.at[k - 1], recv_sem=srecv.at[k - 1],
                                           device_id={"model": lax.rem(me + k, NM)}, device_id_type=MESH) for k in range(1, NM)]
    for c in copies:
        c.start()
    sends += copies
    score_copy.wait_recv()
    sub = lax.broadcasted_iota(jnp.int32, (B, LANES), 0)
    want = jnp.zeros((B, LANES), jnp.int32)
    for b in range(B):
        want = jnp.where(sub == b, rows[b], want)
    lane = lax.broadcasted_iota(jnp.int32, (B, LANES), 1)
    mine = jnp.where(lane + spos * B == want, scb[0, 0:1, :], 0.0)
    theirs = jnp.where(lane + (SPAN - 1 - spos) * B == want, scb[1, 0:1, :], 0.0)
    parent_score = jnp.sum(jnp.where(lane < B, mine + theirs, 0.0), axis=-1, keepdims=True)
    for c in copies:
        c.wait_recv()
    gm = stat[0, 0]
    for k in range(1, NM):
        gm = jnp.maximum(gm, stat[k, 0])
    gs = stat[0, 1] * jnp.exp(stat[0, 0] - gm)
    for k in range(1, NM):
        gs = gs + stat[k, 1] * jnp.exp(stat[k, 0] - gm)
    gm = gm[:, 0:1]
    log_s = jnp.log(gs)[:, 0:1]
    for n in range(NT):
        hi = min((n + 1) * TN, V)
        cand_ref[:, n * TN:hi] = parent_score + ((lgt[n] - gm) - log_s)[:, :hi - n * TN]
    sends.extend(pushes[0])
    for c in sends:
        c.wait_send()


def write_kernel(*refs):
    n = (len(refs) - 1) // 2
    sem = refs[-1]
    copies = []
    for i in range(n):
        src, dst = refs[i], refs[n + i]
        if len(src.shape) > 2:
            copies += [(src.at[j], dst.at[j]) for j in range(src.shape[0])]
        else:
            copies.append((src, dst))
    copies = [pltpu.make_async_copy(a, b, sem.at[j]) for j, (a, b) in enumerate(copies)]
    for c in copies:
        c.start()
    for c in copies:
        c.wait()


def solution(mesh):
    data_beam = ('data', 'beam')
    cache_spec = P(None, data_beam, None, 'model', None)
    col_spec = P(None, None, 'model')
    row_spec = P(None, 'model', None)
    in_specs = (P(data_beam, None), P('data', None), P(), P(data_beam), cache_spec, cache_spec,
                P(), col_spec, col_spec, col_spec, row_spec, P(), col_spec, col_spec, row_spec, P(), P(None, 'model'))
    out_specs = (cache_spec, cache_spec, P(data_beam, 'model'))
    n_model = mesh.shape['model']

    def local_step(x_embed, parent, position, score, k_cache, v_cache, gain_attn, w_query, w_key, w_value, w_out, gain_mlp,
                   w_gate, w_up, w_down, gain_final, w_vocab):
        L, B, S, KH, HD = k_cache.shape
        D = x_embed.shape[1]
        C = KH * HD
        FF = w_gate.shape[2]
        V = w_vocab.shape[1]
        span = parent.shape[1] // B
        half = HD // 2
        freq = np.power(ROPE_BASE, -(np.arange(half, dtype=np.float64) / half)).astype(np.float32)
        freq = jnp.asarray(np.tile(freq, 2 * KH)[None])
        flat = lambda c: jnp.transpose(c, (0, 1, 3, 4, 2)).reshape(L, B, C, S)
        cfg = (L, B, D, HD, S, KH, FF, V, n_model, span)
        any_spec = pl.BlockSpec(memory_space=pl.ANY)
        vm = pl.BlockSpec(memory_space=pltpu.VMEM)
        sm = pl.BlockSpec(memory_space=pltpu.SMEM)
        steps = 2 * L
        NH = 4
        HB = B // NH
        TN = C
        NT = -(-V // TN)
        dma = pltpu.SemaphoreType.DMA
        cache_shape = (L, B, C, S)
        scratch = ([pltpu.VMEM((span * B, C, S), BF16) for _ in range(6)]
                   + [pltpu.VMEM((2, D, C), BF16)] * 3 + [pltpu.VMEM((2, C, D), BF16)]
                   + [pltpu.VMEM((2, D, FF), BF16)] * 2 + [pltpu.VMEM((2, FF, D), BF16)]
                   + [pltpu.VMEM((steps * NH * n_model, HB, D), F32), pltpu.VMEM((n_model, 2, B, LANES), F32), pltpu.VMEM((2, SUB, LANES), F32),
                      pltpu.VMEM((B, D), BF16), pltpu.VMEM((B, C), F32), pltpu.VMEM((B, C), F32),
                      pltpu.VMEM((NH, HB, D), F32), pltpu.VMEM((NH, HB, C), F32), pltpu.VMEM((NH, HB * SUB, S), F32),
                      pltpu.VMEM((NH, HB * SUB, S), F32)] + [pltpu.VMEM((NH, HB, C), F32)] * 3 + [ pltpu.VMEM((NT, B, TN), F32),
                      dma((2 * L,)), dma((14,)), dma((D // S * NT,)), pltpu.SemaphoreType.REGULAR, dma((2 * L,)), dma((2 * L,)),
                      dma((steps * NH * (n_model - 1),)), dma((steps * NH * n_model,)), dma((n_model - 1,)), dma((n_model - 1,)),
                      dma, dma, dma, dma, dma((NH,)), dma((NH,))])
        limit = 64 * 1024 * 1024 - 65536
        outs = pl.pallas_call(
            functools.partial(decode_kernel, cfg),
            out_shape=(pltpu.VMEM(cache_shape, BF16), pltpu.VMEM(cache_shape, BF16), pltpu.VMEM((B, V), F32)),
            in_specs=[sm, sm, vm, vm, vm, vm, vm, vm] + [any_spec] * 10,
            out_specs=(vm, vm, vm),
            scratch_shapes=scratch,
            compiler_params=pltpu.CompilerParams(collective_id=0, has_side_effects=True,
                                                 vmem_limit_bytes=limit - 2 * L * B * C * S * 2 - B * (V + LANES) * 4 - (1 << 19)),
            name="decode_step",
        )(parent, position.reshape(1), x_embed, score[None], freq, gain_attn, gain_mlp, gain_final.reshape(D // LANES, LANES),
          flat(k_cache), flat(v_cache), w_query, w_key, w_value, w_out, w_gate, w_up, w_down, w_vocab.T)
        k_out, v_out, cand = pl.pallas_call(
            write_kernel,
            out_shape=(jax.ShapeDtypeStruct(cache_shape, BF16), jax.ShapeDtypeStruct(cache_shape, BF16),
                       jax.ShapeDtypeStruct((B, V), F32)),
            in_specs=[vm, vm, vm],
            out_specs=(any_spec, any_spec, any_spec),
            scratch_shapes=[dma((2 * L + 1,))],
            compiler_params=pltpu.CompilerParams(vmem_limit_bytes=1 << 20),
            name="write_out",
        )(*outs)
        back = lambda c: jnp.transpose(c.reshape(L, B, KH, HD, S), (0, 1, 4, 2, 3))
        return back(k_out), back(v_out), cand

    return jax.shard_map(local_step, mesh=mesh, in_specs=in_specs, out_specs=out_specs, check_vma=False)
```

```python
import functools

import jax
import jax.numpy as jnp
import numpy as np
from jax import lax
from jax.experimental import pallas as pl
from jax.experimental.pallas import tpu as pltpu
from jax.sharding import PartitionSpec as P

NORM_EPS = 1e-6
ROPE_BASE = 10000.0
MESH = pl.DeviceIdType.MESH
F32 = jnp.float32
BF16 = jnp.bfloat16
LANES = 128
SUB = 8


def rms(res, gain):
    inv = lax.rsqrt(jnp.mean(res * res, axis=-1, keepdims=True) + NORM_EPS)
    return (res * inv * gain.astype(F32)).astype(BF16)


def dot(a, b):
    return jnp.dot(a, b, preferred_element_type=F32)


def dot_t(a, b):
    return lax.dot_general(a, b, (((1,), (1,)), ((), ())), preferred_element_type=F32)


def decode_kernel(cfg, *refs):
    L, B, D, HD, S, KH, FF, V, NM, SPAN = cfg
    (parent_ref, pos_ref, x_ref, score_ref, freq_ref, ga_ref, gm_ref, gf_ref,
     kc, vc, wq, wk, wv, wo, wg, wu, wd, wt, kst, vst, cand_ref,
     kb0, kb1, kb2, vb0, vb1, vb2, wqb, wkb, wvb, wob, wgb, wub, wdb, ar, stat, scb, xb, kn, vn, res, qs, lg, pr, osc, osend, orecv, lgt,
     sem_c, sem_w, sem_t, free, bsend, brecv, asend, arecv, ssend, srecv, csend, crecv, xsend, xrecv, hsend, hrecv) = refs
    slots = [0] + [1 + (l + 1) % 2 for l in range(1, L)]
    kb = [(kb0, kb1, kb2)[j] for j in slots]
    vb = [(vb0, vb1, vb2)[j] for j in slots]
    C = KH * HD
    NH, HB = res.shape[:2]
    me = lax.axis_index("model")
    beam = lax.axis_index("beam")
    spos = lax.rem(beam, SPAN)
    sent = lax.div(beam, SPAN)
    partner = beam - spos + lax.rem(spos + 1, SPAN)
    own = pl.ds(spos * B, B)

    def cache_local(l):
        return (pltpu.make_async_copy(kc.at[l], kb[l].at[own], sem_c.at[2 * l]),
                pltpu.make_async_copy(vc.at[l], vb[l].at[own], sem_c.at[2 * l + 1]))

    def cache_push(l):
        return tuple(pltpu.make_async_remote_copy(src_ref=buf[l].at[own], dst_ref=buf[l].at[own], send_sem=bsend.at[2 * l + i],
                                                  recv_sem=brecv.at[2 * l + i], device_id={"beam": partner}, device_id_type=MESH)
                     for i, buf in enumerate((kb, vb)))

    weights = ((wq, wqb), (wk, wkb), (wv, wvb), (wo, wob), (wg, wgb), (wu, wub), (wd, wdb))

    def weight(l, i):
        src, buf = weights[i]
        return pltpu.make_async_copy(src.at[l], buf.at[l % 2], sem_w.at[(l % 2) * 7 + i])

    chunks = (kb1, vb1, kb2, vb2)
    NCH = D // S
    NT = lgt.shape[0]
    TN = lgt.shape[2]

    def vocab(c, n, rows=TN):
        start = n * TN if isinstance(n, int) else pl.multiple_of(n * TN, TN)
        return pltpu.make_async_copy(wt.at[pl.ds(start, rows), c * S:(c + 1) * S], chunks[c].at[n, pl.ds(0, rows)],
                                     sem_t.at[c * NT + n])

    def vocab_all(which, act):
        def body(n, carry):
            for c in which:
                act(vocab(c, n))
            return carry
        full = V // TN
        lax.fori_loop(0, full, body, 0)
        if full < NT:
            for c in which:
                act(vocab(c, full, V - full * TN))

    for i in range(3):
        weight(0, i).start()
    for c in cache_local(0):
        c.start()

    barrier = pltpu.get_barrier_semaphore()
    for k in range(1, NM):
        pl.semaphore_signal(barrier, inc=1, device_id={"model": lax.rem(me + k, NM)}, device_id_type=MESH)
    pl.semaphore_signal(barrier, inc=1, device_id={"beam": partner}, device_id_type=MESH)

    scb[0] = jnp.zeros((SUB, LANES), F32)
    scb[0, 0:1, 0:B] = score_ref[...]
    pos = pos_ref[0]
    angle = pos.astype(F32) * freq_ref[...]
    cos = jnp.cos(angle)
    sin = jnp.sin(angle)
    rows = [lax.rem(parent_ref[sent, spos * B + b], SPAN * B) for b in range(B)]
    near = [spos * B + lax.rem(r, B) for r in rows]
    far = [spos * B + lax.rem(parent_ref[sent, (SPAN - 1 - spos) * B + b], B) for b in range(B)]

    def rope(x):
        low = lax.rem(lax.broadcasted_iota(jnp.int32, x.shape, 1), HD) < HD // 2
        other = jnp.where(low, -pltpu.roll(x, C - HD // 2, 1), pltpu.roll(x, HD // 2, 1))
        return x * cos + other * sin

    def project(l, r):
        ws = l % 2
        h = rms(r, ga_ref[l:l + 1, :])
        q = rope(dot(h, wqb[ws])).astype(BF16).astype(F32)
        k = rope(dot(h, wkb[ws])).astype(BF16).astype(F32)
        v = dot(h, wvb[ws]).astype(BF16).astype(F32)
        return q * (HD ** -0.5), k, v

    for j in range(3):
        weight(0, j).wait()
    own_q, own_k, own_v = project(0, x_ref[...].astype(F32))
    kn[...] = own_k
    vn[...] = own_v

    pl.semaphore_wait(barrier, NM)

    pushes = [cache_push(l) for l in range(L)]
    x_copy = pltpu.make_async_remote_copy(src_ref=x_ref, dst_ref=xb, send_sem=xsend, recv_sem=xrecv,
                                          device_id={"beam": partner}, device_id_type=MESH)
    x_copy.start()
    score_copy = pltpu.make_async_remote_copy(src_ref=scb.at[0], dst_ref=scb.at[1], send_sem=csend, recv_sem=crecv,
                                              device_id={"beam": partner}, device_id_type=MESH)
    score_copy.start()
    for i in range(3, 7):
        weight(0, i).start()
    for c in cache_local(1):
        c.start()
    for i in range(7):
        weight(1, i).start()

    def peers():
        if NM == 4:
            side = lax.div(me, 2)
            return [3 - 3 * side, 2 - side, me + 1 - 2 * lax.rem(me, 2)]
        return [lax.rem(me + k, NM) for k in range(1, NM)]

    def reduce_copy(step, j, source, peer):
        slot = step * NM + source
        return pltpu.make_async_remote_copy(src_ref=ar.at[slot], dst_ref=ar.at[slot], send_sem=asend.at[step * (NM - 1) + j],
                                            recv_sem=arecv.at[slot], device_id={"model": peer}, device_id_type=MESH)

    def reduce_start(step, value):
        ar[step * NM + me] = value
        copies = [reduce_copy(step, j, me, peer) for j, peer in enumerate(peers())]
        for c in copies:
            c.start()
        sends.extend(copies)
        return step

    def reduce_finish(step):
        for k in range(1, NM):
            reduce_copy(step, 0, lax.rem(me + k, NM), me).wait_recv()
        total = ar[step * NM]
        for k in range(1, NM):
            total = total + ar[step * NM + k]
        return total

    head_of_lane = lax.broadcasted_iota(jnp.int32, (SUB, C), 1) // HD
    head_mask = head_of_lane == lax.broadcasted_iota(jnp.int32, (SUB, C), 0)
    here = lax.broadcasted_iota(jnp.int32, (C, S), 1) == pos
    sends = [score_copy, x_copy]

    def columns(x):
        return jnp.concatenate([x, jnp.zeros((LANES - x.shape[0], C), F32)], axis=0).T

    def insert(cols, b, row):
        return jnp.where(here, jnp.broadcast_to(cols[:, b:b + 1], (C, S)).astype(BF16), row)

    def attention(l, i, q, k, v, index, out, keep, ready):
        qs[i] = q
        k_cols = columns(k)
        v_cols = columns(v)
        ready(0)
        for b in range(HB):
            kept = insert(k_cols, b, kb[l][index[i * HB + b]])
            if keep:
                kst[l, i * HB + b] = kept
            qb = jnp.where(head_mask, jnp.broadcast_to(qs[i, b:b + 1, :], (SUB, C)), 0.0).astype(BF16)
            lg[i, b * SUB:(b + 1) * SUB, :] = dot(qb, kept)
        logits = lg[i]
        logits = jnp.where(lax.broadcasted_iota(jnp.int32, logits.shape, 1) <= pos, logits, -jnp.inf)
        e = jnp.exp(logits - jnp.max(logits, axis=-1, keepdims=True))
        pr[i] = e / jnp.sum(e, axis=-1, keepdims=True)
        ready(1)
        for b in range(HB):
            kept = insert(v_cols, b, vb[l][index[i * HB + b]])
            if keep:
                vst[l, i * HB + b] = kept
            ob = dot_t(pr[i, b * SUB:(b + 1) * SUB, :].astype(BF16), kept)
            out[i, b:b + 1, :] = jnp.sum(jnp.where(head_mask, ob, 0.0), axis=0, keepdims=True)

    def project_out(l, i, o):
        if i == 0:
            weight(l, 3).wait()
        return reduce_start(2 * l * NH + i, dot(o.astype(BF16), wob[l % 2]))

    def attend(l, i, r):
        if i == 0:
            for j in range(3):
                weight(l, j).wait()
        q, k, v = project(l, r)

        def ready(which):
            if i == 0:
                pushes[l][which].wait_recv()

        attention(l, i, q, k, v, rows, osc, True, ready)
        return project_out(l, i, osc[i])

    def attend_first():
        for c in cache_local(0):
            c.wait()
        part = lambda x, i: x[i * HB:(i + 1) * HB, :]
        for i in range(NH):
            attention(0, i, part(own_q, i), part(own_k, i), part(own_v, i), near, osc, False, lambda w: None)
        x_copy.wait_recv()
        q, k, v = project(0, xb[...].astype(F32))
        copies = []
        for i in range(NH):
            attention(0, i, part(q, i), part(k, i), part(v, i), far, osend, False, lambda w: None)
            copies.append(pltpu.make_async_remote_copy(src_ref=osend.at[i], dst_ref=orecv.at[i], send_sem=hsend.at[i], recv_sem=hrecv.at[i],
                                                       device_id={"beam": partner}, device_id_type=MESH))
            copies[i].start()
        sends.extend(copies)
        steps = []
        for i in range(NH):
            copies[i].wait_recv()
            home = jnp.zeros((HB, C), jnp.int32)
            for b in range(HB):
                home = jnp.where(lax.broadcasted_iota(jnp.int32, (HB, C), 0) == b, lax.div(rows[i * HB + b], B), home)
            steps.append(project_out(0, i, jnp.where(home == spos, osc[i], orecv[i])))
        return steps

    def keep_first(which):
        cols = columns((kn, vn)[which][...])
        pushes[0][which].wait_recv()
        for b in range(B):
            (kst, vst)[which][0, b] = insert(cols, b, (kb, vb)[which][0][rows[b]])

    def mlp(l, i, r):
        ws = l % 2
        h = rms(r, gm_ref[l:l + 1, :])
        if i == 0:
            weight(l, 4).wait()
            weight(l, 5).wait()
        gate = dot(h, wgb[ws])
        up = dot(h, wub[ws])
        g = (gate * jax.nn.sigmoid(gate) * up).astype(BF16)
        if i == 0:
            weight(l, 6).wait()
        return reduce_start((2 * l + 1) * NH + i, dot(g, wdb[ws]))

    for i in range(NH):
        res[i] = x_ref[i * HB:(i + 1) * HB, :].astype(F32)
    def push(l, which):
        if l > 0:
            cache_local(l)[which].wait()
        pushes[l][which].start()

    started = attend_first()
    order = [(1, 0), (1, 1)] + [(l, w) for l in range(2, L) for w in range(2)] + [(0, 0), (0, 1)]
    order = [order[:2]] + [[o] for o in order[2:]]
    for l in range(L):
        if l > 0:
            for i in range(NH):
                res[i] = res[i] + reduce_finish(started[i])
                started[i] = attend(l, i, res[i])
            if l + 2 < L:
                pl.semaphore_signal(free, inc=1, device_id={"beam": partner}, device_id_type=MESH)
        for o in order[2 * l] if 2 * l < len(order) else []:
            push(*o)
        if l + 2 < L:
            for which in range(2):
                if l > 0:
                    pushes[l][which].wait_send()
                cache_local(l + 2)[which].start()
            for j in range(4):
                weight(l + 2, j).start()
        if l == L - 1:
            for j in (l - 1, l):
                for which in range(2):
                    pushes[j][which].wait_send()
            vocab_all(range(NCH), lambda c: c.start())
            keep_first(0)
        for i in range(NH):
            res[i] = res[i] + reduce_finish(started[i])
            started[i] = mlp(l, i, res[i])
        for o in order[2 * l + 1] if 2 * l + 1 < len(order) else []:
            if o[0] >= 3 and o[1] == 0:
                pl.semaphore_wait(free, 1)
            push(*o)
        if l + 2 < L:
            for j in range(4, 7):
                weight(l + 2, j).start()
        if l == L - 1:
            keep_first(1)
    for i in range(NH):
        res[i] = res[i] + reduce_finish(started[i])

    gf = gf_ref[...].astype(F32)
    h = rms(jnp.concatenate([res[i] for i in range(NH)], axis=0), jnp.concatenate([gf[i:i + 1, :] for i in range(D // LANES)], axis=1))
    vocab_all(range(NCH), lambda c: c.wait())

    def tile(n, carry):
        acc = dot_t(h[:, 0:S], chunks[0][n])
        for c in range(1, NCH):
            acc = acc + dot_t(h[:, c * S:(c + 1) * S], chunks[c][n])
        acc = jnp.where(lax.broadcasted_iota(jnp.int32, (B, TN), 1) + n * TN < V, acc, -jnp.inf)
        lgt[n] = acc
        return jnp.maximum(carry, acc)

    peak = lax.fori_loop(0, NT, tile, jnp.full((B, TN), -jnp.inf, F32))
    m = jnp.max(peak, axis=-1, keepdims=True)

    def add_exp(n, carry):
        return carry + jnp.exp(lgt[n] - m)

    s = jnp.sum(lax.fori_loop(0, NT, add_exp, jnp.zeros((B, TN), F32)), axis=-1, keepdims=True)
    stat[me, 0] = jnp.broadcast_to(m, (B, LANES))
    stat[me, 1] = jnp.broadcast_to(s, (B, LANES))
    copies = [pltpu.make_async_remote_copy(src_ref=stat.at[me], dst_ref=stat.at[me], send_sem=ssend.at[k - 1], recv_sem=srecv.at[k - 1],
                                           device_id={"model": lax.rem(me + k, NM)}, device_id_type=MESH) for k in range(1, NM)]
    for c in copies:
        c.start()
    sends += copies
    score_copy.wait_recv()
    sub = lax.broadcasted_iota(jnp.int32, (B, LANES), 0)
    want = jnp.zeros((B, LANES), jnp.int32)
    for b in range(B):
        want = jnp.where(sub == b, rows[b], want)
    lane = lax.broadcasted_iota(jnp.int32, (B, LANES), 1)
    mine = jnp.where(lane + spos * B == want, scb[0, 0:1, :], 0.0)
    theirs = jnp.where(lane + (SPAN - 1 - spos) * B == want, scb[1, 0:1, :], 0.0)
    parent_score = jnp.sum(jnp.where(lane < B, mine + theirs, 0.0), axis=-1, keepdims=True)
    for c in copies:
        c.wait_recv()
    gm = stat[0, 0]
    for k in range(1, NM):
        gm = jnp.maximum(gm, stat[k, 0])
    gs = stat[0, 1] * jnp.exp(stat[0, 0] - gm)
    for k in range(1, NM):
        gs = gs + stat[k, 1] * jnp.exp(stat[k, 0] - gm)
    gm = gm[:, 0:1]
    log_s = jnp.log(gs)[:, 0:1]
    for n in range(NT):
        hi = min((n + 1) * TN, V)
        cand_ref[:, n * TN:hi] = parent_score + ((lgt[n] - gm) - log_s)[:, :hi - n * TN]
    sends.extend(pushes[0])
    for c in sends:
        c.wait_send()


def write_kernel(*refs):
    n = (len(refs) - 1) // 2
    sem = refs[-1]
    copies = []
    for i in range(n):
        src, dst = refs[i], refs[n + i]
        if len(src.shape) > 2:
            copies += [(src.at[j], dst.at[j]) for j in range(src.shape[0])]
        else:
            copies.append((src, dst))
    copies = [pltpu.make_async_copy(a, b, sem.at[j]) for j, (a, b) in enumerate(copies)]
    for c in copies:
        c.start()
    for c in copies:
        c.wait()


def solution(mesh):
    data_beam = ('data', 'beam')
    cache_spec = P(None, data_beam, None, 'model', None)
    col_spec = P(None, None, 'model')
    row_spec = P(None, 'model', None)
    in_specs = (P(data_beam, None), P('data', None), P(), P(data_beam), cache_spec, cache_spec,
                P(), col_spec, col_spec, col_spec, row_spec, P(), col_spec, col_spec, row_spec, P(), P(None, 'model'))
    out_specs = (cache_spec, cache_spec, P(data_beam, 'model'))
    n_model = mesh.shape['model']

    def local_step(x_embed, parent, position, score, k_cache, v_cache, gain_attn, w_query, w_key, w_value, w_out, gain_mlp,
                   w_gate, w_up, w_down, gain_final, w_vocab):
        L, B, S, KH, HD = k_cache.shape
        D = x_embed.shape[1]
        C = KH * HD
        FF = w_gate.shape[2]
        V = w_vocab.shape[1]
        span = parent.shape[1] // B
        half = HD // 2
        freq = np.power(ROPE_BASE, -(np.arange(half, dtype=np.float64) / half)).astype(np.float32)
        freq = jnp.asarray(np.tile(freq, 2 * KH)[None])
        flat = lambda c: jnp.transpose(c, (0, 1, 3, 4, 2)).reshape(L, B, C, S)
        cfg = (L, B, D, HD, S, KH, FF, V, n_model, span)
        any_spec = pl.BlockSpec(memory_space=pl.ANY)
        vm = pl.BlockSpec(memory_space=pltpu.VMEM)
        sm = pl.BlockSpec(memory_space=pltpu.SMEM)
        steps = 2 * L
        NH = 2
        HB = B // NH
        TN = C
        NT = -(-V // TN)
        dma = pltpu.SemaphoreType.DMA
        cache_shape = (L, B, C, S)
        scratch = ([pltpu.VMEM((span * B, C, S), BF16) for _ in range(6)]
                   + [pltpu.VMEM((2, D, C), BF16)] * 3 + [pltpu.VMEM((2, C, D), BF16)]
                   + [pltpu.VMEM((2, D, FF), BF16)] * 2 + [pltpu.VMEM((2, FF, D), BF16)]
                   + [pltpu.VMEM((steps * NH * n_model, HB, D), F32), pltpu.VMEM((n_model, 2, B, LANES), F32), pltpu.VMEM((2, SUB, LANES), F32),
                      pltpu.VMEM((B, D), BF16), pltpu.VMEM((B, C), F32), pltpu.VMEM((B, C), F32),
                      pltpu.VMEM((NH, HB, D), F32), pltpu.VMEM((NH, HB, C), F32), pltpu.VMEM((NH, HB * SUB, S), F32),
                      pltpu.VMEM((NH, HB * SUB, S), F32)] + [pltpu.VMEM((NH, HB, C), F32)] * 3 + [ pltpu.VMEM((NT, B, TN), F32),
                      dma((2 * L,)), dma((14,)), dma((D // S * NT,)), pltpu.SemaphoreType.REGULAR, dma((2 * L,)), dma((2 * L,)),
                      dma((steps * NH * (n_model - 1),)), dma((steps * NH * n_model,)), dma((n_model - 1,)), dma((n_model - 1,)),
                      dma, dma, dma, dma, dma((NH,)), dma((NH,))])
        limit = 64 * 1024 * 1024 - 65536
        outs = pl.pallas_call(
            functools.partial(decode_kernel, cfg),
            out_shape=(pltpu.VMEM(cache_shape, BF16), pltpu.VMEM(cache_shape, BF16), pltpu.VMEM((B, V), F32)),
            in_specs=[sm, sm, vm, vm, vm, vm, vm, vm] + [any_spec] * 10,
            out_specs=(vm, vm, vm),
            scratch_shapes=scratch,
            compiler_params=pltpu.CompilerParams(collective_id=0, has_side_effects=True,
                                                 vmem_limit_bytes=limit - 2 * L * B * C * S * 2 - B * (V + LANES) * 4 - (1 << 19)),
            name="decode_step",
        )(parent, position.reshape(1), x_embed, score[None], freq, gain_attn, gain_mlp, gain_final.reshape(D // LANES, LANES),
          flat(k_cache), flat(v_cache), w_query, w_key, w_value, w_out, w_gate, w_up, w_down, w_vocab.T)
        k_out, v_out, cand = pl.pallas_call(
            write_kernel,
            out_shape=(jax.ShapeDtypeStruct(cache_shape, BF16), jax.ShapeDtypeStruct(cache_shape, BF16),
                       jax.ShapeDtypeStruct((B, V), F32)),
            in_specs=[vm, vm, vm],
            out_specs=(any_spec, any_spec, any_spec),
            scratch_shapes=[dma((2 * L + 1,))],
            compiler_params=pltpu.CompilerParams(vmem_limit_bytes=1 << 20),
            name="write_out",
        )(*outs)
        back = lambda c: jnp.transpose(c.reshape(L, B, KH, HD, S), (0, 1, 4, 2, 3))
        return back(k_out), back(v_out), cand

    return jax.shard_map(local_step, mesh=mesh, in_specs=in_specs, out_specs=out_specs, check_vma=False)
```

```python
import functools

import jax
import jax.numpy as jnp
import numpy as np
from jax import lax
from jax.experimental import pallas as pl
from jax.experimental.pallas import tpu as pltpu
from jax.sharding import PartitionSpec as P

NORM_EPS = 1e-6
ROPE_BASE = 10000.0
MESH = pl.DeviceIdType.MESH
F32 = jnp.float32
BF16 = jnp.bfloat16
LANES = 128
SUB = 8


def rms(res, gain):
    inv = lax.rsqrt(jnp.mean(res * res, axis=-1, keepdims=True) + NORM_EPS)
    return (res * inv * gain.astype(F32)).astype(BF16)


def dot(a, b):
    return jnp.dot(a, b, preferred_element_type=F32)


def dot_t(a, b):
    return lax.dot_general(a, b, (((1,), (1,)), ((), ())), preferred_element_type=F32)


def decode_kernel(cfg, *refs):
    L, B, D, HD, S, KH, FF, V, NM, SPAN = cfg
    (parent_ref, pos_ref, x_ref, score_ref, freq_ref, ga_ref, gm_ref, gf_ref,
     kc, vc, wq, wk, wv, wo, wg, wu, wd, wt, kst, vst, cand_ref,
     kb0, kb1, kb2, vb0, vb1, vb2, wqb, wkb, wvb, wob, wgb, wub, wdb, ar, stat, scb, xb, kn, vn, res, qs, lg, pr, osc, osend, orecv, lgt,
     sem_c, sem_w, sem_t, free, bsend, brecv, asend, arecv, ssend, srecv, csend, crecv, xsend, xrecv, hsend, hrecv) = refs
    slots = [0] + [1 + (l + 1) % 2 for l in range(1, L)]
    kb = [(kb0, kb1, kb2)[j] for j in slots]
    vb = [(vb0, vb1, vb2)[j] for j in slots]
    C = KH * HD
    NH, HB = res.shape[:2]
    NP = bsend.shape[0] // (2 * L)
    me = lax.axis_index("model")
    beam = lax.axis_index("beam")
    spos = lax.rem(beam, SPAN)
    sent = lax.div(beam, SPAN)
    partner = beam - spos + lax.rem(spos + 1, SPAN)
    own = pl.ds(spos * B, B)

    def cache_local(l):
        return (pltpu.make_async_copy(kc.at[l], kb[l].at[own], sem_c.at[2 * l]),
                pltpu.make_async_copy(vc.at[l], vb[l].at[own], sem_c.at[2 * l + 1]))

    def cache_push(l, which, j):
        buf = (kb, vb)[which][l].at[pl.ds(spos * B + j * (B // NP), B // NP)]
        n = (2 * l + which) * NP + j
        return pltpu.make_async_remote_copy(src_ref=buf, dst_ref=buf, send_sem=bsend.at[n], recv_sem=brecv.at[n],
                                            device_id={"beam": partner}, device_id_type=MESH)

    weights = ((wq, wqb), (wk, wkb), (wv, wvb), (wo, wob), (wg, wgb), (wu, wub), (wd, wdb))

    def weight(l, i):
        src, buf = weights[i]
        return pltpu.make_async_copy(src.at[l], buf.at[l % 2], sem_w.at[(l % 2) * 7 + i])

    chunks = (kb1, vb1, kb2, vb2)
    NCH = D // S
    NT = lgt.shape[0]
    TN = lgt.shape[2]

    def vocab(c, n, rows=TN):
        start = n * TN if isinstance(n, int) else pl.multiple_of(n * TN, TN)
        return pltpu.make_async_copy(wt.at[pl.ds(start, rows), c * S:(c + 1) * S], chunks[c].at[n, pl.ds(0, rows)],
                                     sem_t.at[c * NT + n])

    def vocab_all(which, act):
        def body(n, carry):
            for c in which:
                act(vocab(c, n))
            return carry
        full = V // TN
        lax.fori_loop(0, full, body, 0)
        if full < NT:
            for c in which:
                act(vocab(c, full, V - full * TN))

    for i in range(3):
        weight(0, i).start()
    for c in cache_local(0):
        c.start()

    barrier = pltpu.get_barrier_semaphore()
    for k in range(1, NM):
        pl.semaphore_signal(barrier, inc=1, device_id={"model": lax.rem(me + k, NM)}, device_id_type=MESH)
    pl.semaphore_signal(barrier, inc=1, device_id={"beam": partner}, device_id_type=MESH)

    scb[0] = jnp.zeros((SUB, LANES), F32)
    scb[0, 0:1, 0:B] = score_ref[...]
    pos = pos_ref[0]
    angle = pos.astype(F32) * freq_ref[...]
    cos = jnp.cos(angle)
    sin = jnp.sin(angle)
    rows = [lax.rem(parent_ref[sent, spos * B + b], SPAN * B) for b in range(B)]
    near = [spos * B + lax.rem(r, B) for r in rows]
    far = [spos * B + lax.rem(parent_ref[sent, (SPAN - 1 - spos) * B + b], B) for b in range(B)]

    def rope(x):
        low = lax.rem(lax.broadcasted_iota(jnp.int32, x.shape, 1), HD) < HD // 2
        other = jnp.where(low, -pltpu.roll(x, C - HD // 2, 1), pltpu.roll(x, HD // 2, 1))
        return x * cos + other * sin

    def project(l, r):
        ws = l % 2
        h = rms(r, ga_ref[l:l + 1, :])
        q = rope(dot(h, wqb[ws])).astype(BF16).astype(F32)
        k = rope(dot(h, wkb[ws])).astype(BF16).astype(F32)
        v = dot(h, wvb[ws]).astype(BF16).astype(F32)
        return q * (HD ** -0.5), k, v

    for j in range(3):
        weight(0, j).wait()
    own_q, own_k, own_v = project(0, x_ref[...].astype(F32))
    kn[...] = own_k
    vn[...] = own_v

    pl.semaphore_wait(barrier, NM)

    pushes = [[[cache_push(l, which, j) for j in range(NP)] for which in range(2)] for l in range(L)]
    x_copy = pltpu.make_async_remote_copy(src_ref=x_ref, dst_ref=xb, send_sem=xsend, recv_sem=xrecv,
                                          device_id={"beam": partner}, device_id_type=MESH)
    x_copy.start()
    score_copy = pltpu.make_async_remote_copy(src_ref=scb.at[0], dst_ref=scb.at[1], send_sem=csend, recv_sem=crecv,
                                              device_id={"beam": partner}, device_id_type=MESH)
    score_copy.start()
    for i in range(3, 7):
        weight(0, i).start()
    for c in cache_local(1):
        c.start()
    for i in range(7):
        weight(1, i).start()

    def peers():
        if NM == 4:
            side = lax.div(me, 2)
            return [3 - 3 * side, 2 - side, me + 1 - 2 * lax.rem(me, 2)]
        return [lax.rem(me + k, NM) for k in range(1, NM)]

    def reduce_copy(step, j, source, peer):
        slot = step * NM + source
        return pltpu.make_async_remote_copy(src_ref=ar.at[slot], dst_ref=ar.at[slot], send_sem=asend.at[step * (NM - 1) + j],
                                            recv_sem=arecv.at[slot], device_id={"model": peer}, device_id_type=MESH)

    def reduce_start(step, value):
        ar[step * NM + me] = value
        copies = [reduce_copy(step, j, me, peer) for j, peer in enumerate(peers())]
        for c in copies:
            c.start()
        sends.extend(copies)
        return step

    def reduce_finish(step):
        for k in range(1, NM):
            reduce_copy(step, 0, lax.rem(me + k, NM), me).wait_recv()
        total = ar[step * NM]
        for k in range(1, NM):
            total = total + ar[step * NM + k]
        return total

    head_of_lane = lax.broadcasted_iota(jnp.int32, (SUB, C), 1) // HD
    head_mask = head_of_lane == lax.broadcasted_iota(jnp.int32, (SUB, C), 0)
    here = lax.broadcasted_iota(jnp.int32, (C, S), 1) == pos
    sends = [score_copy, x_copy]

    def columns(x):
        return jnp.concatenate([x, jnp.zeros((LANES - x.shape[0], C), F32)], axis=0).T

    def insert(cols, b, row):
        return jnp.where(here, jnp.broadcast_to(cols[:, b:b + 1], (C, S)).astype(BF16), row)

    def attention(l, i, q, k, v, index, out, keep, ready):
        qs[i] = q
        k_cols = columns(k)
        v_cols = columns(v)
        ready(0)
        for b in range(HB):
            kept = insert(k_cols, b, kb[l][index[i * HB + b]])
            if keep:
                kst[l, i * HB + b] = kept
            qb = jnp.where(head_mask, jnp.broadcast_to(qs[i, b:b + 1, :], (SUB, C)), 0.0).astype(BF16)
            lg[i, b * SUB:(b + 1) * SUB, :] = dot(qb, kept)
        logits = lg[i]
        logits = jnp.where(lax.broadcasted_iota(jnp.int32, logits.shape, 1) <= pos, logits, -jnp.inf)
        e = jnp.exp(logits - jnp.max(logits, axis=-1, keepdims=True))
        pr[i] = e / jnp.sum(e, axis=-1, keepdims=True)
        ready(1)
        for b in range(HB):
            kept = insert(v_cols, b, vb[l][index[i * HB + b]])
            if keep:
                vst[l, i * HB + b] = kept
            ob = dot_t(pr[i, b * SUB:(b + 1) * SUB, :].astype(BF16), kept)
            out[i, b:b + 1, :] = jnp.sum(jnp.where(head_mask, ob, 0.0), axis=0, keepdims=True)

    def project_out(l, i, o):
        if i == 0:
            weight(l, 3).wait()
        return reduce_start(2 * l * NH + i, dot(o.astype(BF16), wob[l % 2]))

    def attend(l, i, r):
        if i == 0:
            for j in range(3):
                weight(l, j).wait()
        q, k, v = project(l, r)

        def ready(which):
            if i == 0:
                for c in pushes[l][which]:
                    c.wait_recv()

        attention(l, i, q, k, v, rows, osc, True, ready)
        return project_out(l, i, osc[i])

    def attend_first():
        for c in cache_local(0):
            c.wait()
        part = lambda x, i: x[i * HB:(i + 1) * HB, :]
        for i in range(NH):
            attention(0, i, part(own_q, i), part(own_k, i), part(own_v, i), near, osc, False, lambda w: None)
        x_copy.wait_recv()
        q, k, v = project(0, xb[...].astype(F32))
        copies = []
        for i in range(NH):
            attention(0, i, part(q, i), part(k, i), part(v, i), far, osend, False, lambda w: None)
            copies.append(pltpu.make_async_remote_copy(src_ref=osend.at[i], dst_ref=orecv.at[i], send_sem=hsend.at[i], recv_sem=hrecv.at[i],
                                                       device_id={"beam": partner}, device_id_type=MESH))
            copies[i].start()
        sends.extend(copies)
        steps = []
        for i in range(NH):
            copies[i].wait_recv()
            home = jnp.zeros((HB, C), jnp.int32)
            for b in range(HB):
                home = jnp.where(lax.broadcasted_iota(jnp.int32, (HB, C), 0) == b, lax.div(rows[i * HB + b], B), home)
            steps.append(project_out(0, i, jnp.where(home == spos, osc[i], orecv[i])))
        return steps

    def keep_first(which):
        cols = columns((kn, vn)[which][...])
        for c in pushes[0][which]:
            c.wait_recv()
        for b in range(B):
            (kst, vst)[which][0, b] = insert(cols, b, (kb, vb)[which][0][rows[b]])

    def mlp(l, i, r):
        ws = l % 2
        h = rms(r, gm_ref[l:l + 1, :])
        if i == 0:
            weight(l, 4).wait()
            weight(l, 5).wait()
        gate = dot(h, wgb[ws])
        up = dot(h, wub[ws])
        g = (gate * jax.nn.sigmoid(gate) * up).astype(BF16)
        if i == 0:
            weight(l, 6).wait()
        return reduce_start((2 * l + 1) * NH + i, dot(g, wdb[ws]))

    for i in range(NH):
        res[i] = x_ref[i * HB:(i + 1) * HB, :].astype(F32)
    queue = [(l, which, j) for l in list(range(1, L)) + [0] for which in range(2) for j in range(NP)]

    def feed(count):
        for _ in range(min(count, len(queue))):
            l, which, j = queue.pop(0)
            if j == 0 and l > 0:
                if l >= 3 and which == 0:
                    pl.semaphore_wait(free, 1)
                cache_local(l)[which].wait()
            pushes[l][which][j].start()

    started = attend_first()
    for l in range(L):
        if l > 0:
            for i in range(NH):
                res[i] = res[i] + reduce_finish(started[i])
                started[i] = attend(l, i, res[i])
                feed(NP // NH)
            if l + 2 < L:
                pl.semaphore_signal(free, inc=1, device_id={"beam": partner}, device_id_type=MESH)
        else:
            feed(NP + NP // 2)
        if l + 2 < L:
            for which in range(2):
                if l > 0:
                    for c in pushes[l][which]:
                        c.wait_send()
                cache_local(l + 2)[which].start()
            for j in range(4):
                weight(l + 2, j).start()
        if l == L - 1:
            for j in (l - 1, l):
                for which in range(2):
                    for c in pushes[j][which]:
                        c.wait_send()
            vocab_all(range(NCH), lambda c: c.start())
            keep_first(0)
        for i in range(NH):
            res[i] = res[i] + reduce_finish(started[i])
            started[i] = mlp(l, i, res[i])
            feed(NP // NH)
        if l + 2 < L:
            for j in range(4, 7):
                weight(l + 2, j).start()
        if l == L - 1:
            feed(len(queue))
            keep_first(1)
    for i in range(NH):
        res[i] = res[i] + reduce_finish(started[i])

    gf = gf_ref[...].astype(F32)
    h = rms(jnp.concatenate([res[i] for i in range(NH)], axis=0), jnp.concatenate([gf[i:i + 1, :] for i in range(D // LANES)], axis=1))
    vocab_all(range(NCH), lambda c: c.wait())

    def tile(n, carry):
        acc = dot_t(h[:, 0:S], chunks[0][n])
        for c in range(1, NCH):
            acc = acc + dot_t(h[:, c * S:(c + 1) * S], chunks[c][n])
        acc = jnp.where(lax.broadcasted_iota(jnp.int32, (B, TN), 1) + n * TN < V, acc, -jnp.inf)
        lgt[n] = acc
        return jnp.maximum(carry, acc)

    peak = lax.fori_loop(0, NT, tile, jnp.full((B, TN), -jnp.inf, F32))
    m = jnp.max(peak, axis=-1, keepdims=True)

    def add_exp(n, carry):
        return carry + jnp.exp(lgt[n] - m)

    s = jnp.sum(lax.fori_loop(0, NT, add_exp, jnp.zeros((B, TN), F32)), axis=-1, keepdims=True)
    stat[me, 0] = jnp.broadcast_to(m, (B, LANES))
    stat[me, 1] = jnp.broadcast_to(s, (B, LANES))
    copies = [pltpu.make_async_remote_copy(src_ref=stat.at[me], dst_ref=stat.at[me], send_sem=ssend.at[k - 1], recv_sem=srecv.at[k - 1],
                                           device_id={"model": lax.rem(me + k, NM)}, device_id_type=MESH) for k in range(1, NM)]
    for c in copies:
        c.start()
    sends += copies
    score_copy.wait_recv()
    sub = lax.broadcasted_iota(jnp.int32, (B, LANES), 0)
    want = jnp.zeros((B, LANES), jnp.int32)
    for b in range(B):
        want = jnp.where(sub == b, rows[b], want)
    lane = lax.broadcasted_iota(jnp.int32, (B, LANES), 1)
    mine = jnp.where(lane + spos * B == want, scb[0, 0:1, :], 0.0)
    theirs = jnp.where(lane + (SPAN - 1 - spos) * B == want, scb[1, 0:1, :], 0.0)
    parent_score = jnp.sum(jnp.where(lane < B, mine + theirs, 0.0), axis=-1, keepdims=True)
    for c in copies:
        c.wait_recv()
    gm = stat[0, 0]
    for k in range(1, NM):
        gm = jnp.maximum(gm, stat[k, 0])
    gs = stat[0, 1] * jnp.exp(stat[0, 0] - gm)
    for k in range(1, NM):
        gs = gs + stat[k, 1] * jnp.exp(stat[k, 0] - gm)
    gm = gm[:, 0:1]
    log_s = jnp.log(gs)[:, 0:1]
    for n in range(NT):
        hi = min((n + 1) * TN, V)
        cand_ref[:, n * TN:hi] = parent_score + ((lgt[n] - gm) - log_s)[:, :hi - n * TN]
    sends.extend(pushes[0][0] + pushes[0][1])
    for c in sends:
        c.wait_send()


def write_kernel(*refs):
    n = (len(refs) - 1) // 2
    sem = refs[-1]
    copies = []
    for i in range(n):
        src, dst = refs[i], refs[n + i]
        if len(src.shape) > 2:
            copies += [(src.at[j], dst.at[j]) for j in range(src.shape[0])]
        else:
            copies.append((src, dst))
    copies = [pltpu.make_async_copy(a, b, sem.at[j]) for j, (a, b) in enumerate(copies)]
    for c in copies:
        c.start()
    for c in copies:
        c.wait()


def solution(mesh):
    data_beam = ('data', 'beam')
    cache_spec = P(None, data_beam, None, 'model', None)
    col_spec = P(None, None, 'model')
    row_spec = P(None, 'model', None)
    in_specs = (P(data_beam, None), P('data', None), P(), P(data_beam), cache_spec, cache_spec,
                P(), col_spec, col_spec, col_spec, row_spec, P(), col_spec, col_spec, row_spec, P(), P(None, 'model'))
    out_specs = (cache_spec, cache_spec, P(data_beam, 'model'))
    n_model = mesh.shape['model']

    def local_step(x_embed, parent, position, score, k_cache, v_cache, gain_attn, w_query, w_key, w_value, w_out, gain_mlp,
                   w_gate, w_up, w_down, gain_final, w_vocab):
        L, B, S, KH, HD = k_cache.shape
        D = x_embed.shape[1]
        C = KH * HD
        FF = w_gate.shape[2]
        V = w_vocab.shape[1]
        span = parent.shape[1] // B
        half = HD // 2
        freq = np.power(ROPE_BASE, -(np.arange(half, dtype=np.float64) / half)).astype(np.float32)
        freq = jnp.asarray(np.tile(freq, 2 * KH)[None])
        flat = lambda c: jnp.transpose(c, (0, 1, 3, 4, 2)).reshape(L, B, C, S)
        cfg = (L, B, D, HD, S, KH, FF, V, n_model, span)
        any_spec = pl.BlockSpec(memory_space=pl.ANY)
        vm = pl.BlockSpec(memory_space=pltpu.VMEM)
        sm = pl.BlockSpec(memory_space=pltpu.SMEM)
        steps = 2 * L
        NH = 4
        NP = 4
        HB = B // NH
        TN = C
        NT = -(-V // TN)
        dma = pltpu.SemaphoreType.DMA
        cache_shape = (L, B, C, S)
        scratch = ([pltpu.VMEM((span * B, C, S), BF16) for _ in range(6)]
                   + [pltpu.VMEM((2, D, C), BF16)] * 3 + [pltpu.VMEM((2, C, D), BF16)]
                   + [pltpu.VMEM((2, D, FF), BF16)] * 2 + [pltpu.VMEM((2, FF, D), BF16)]
                   + [pltpu.VMEM((steps * NH * n_model, HB, D), F32), pltpu.VMEM((n_model, 2, B, LANES), F32), pltpu.VMEM((2, SUB, LANES), F32),
                      pltpu.VMEM((B, D), BF16), pltpu.VMEM((B, C), F32), pltpu.VMEM((B, C), F32),
                      pltpu.VMEM((NH, HB, D), F32), pltpu.VMEM((NH, HB, C), F32), pltpu.VMEM((NH, HB * SUB, S), F32),
                      pltpu.VMEM((NH, HB * SUB, S), F32)] + [pltpu.VMEM((NH, HB, C), F32)] * 3 + [ pltpu.VMEM((NT, B, TN), F32),
                      dma((2 * L,)), dma((14,)), dma((D // S * NT,)), pltpu.SemaphoreType.REGULAR, dma((2 * L * NP,)), dma((2 * L * NP,)),
                      dma((steps * NH * (n_model - 1),)), dma((steps * NH * n_model,)), dma((n_model - 1,)), dma((n_model - 1,)),
                      dma, dma, dma, dma, dma((NH,)), dma((NH,))])
        limit = 64 * 1024 * 1024 - 65536
        outs = pl.pallas_call(
            functools.partial(decode_kernel, cfg),
            out_shape=(pltpu.VMEM(cache_shape, BF16), pltpu.VMEM(cache_shape, BF16), pltpu.VMEM((B, V), F32)),
            in_specs=[sm, sm, vm, vm, vm, vm, vm, vm] + [any_spec] * 10,
            out_specs=(vm, vm, vm),
            scratch_shapes=scratch,
            compiler_params=pltpu.CompilerParams(collective_id=0, has_side_effects=True,
                                                 vmem_limit_bytes=limit - 2 * L * B * C * S * 2 - B * (V + LANES) * 4 - (1 << 19)),
            name="decode_step",
        )(parent, position.reshape(1), x_embed, score[None], freq, gain_attn, gain_mlp, gain_final.reshape(D // LANES, LANES),
          flat(k_cache), flat(v_cache), w_query, w_key, w_value, w_out, w_gate, w_up, w_down, w_vocab.T)
        k_out, v_out, cand = pl.pallas_call(
            write_kernel,
            out_shape=(jax.ShapeDtypeStruct(cache_shape, BF16), jax.ShapeDtypeStruct(cache_shape, BF16),
                       jax.ShapeDtypeStruct((B, V), F32)),
            in_specs=[vm, vm, vm],
            out_specs=(any_spec, any_spec, any_spec),
            scratch_shapes=[dma((2 * L + 1,))],
            compiler_params=pltpu.CompilerParams(vmem_limit_bytes=1 << 20),
            name="write_out",
        )(*outs)
        back = lambda c: jnp.transpose(c.reshape(L, B, KH, HD, S), (0, 1, 4, 2, 3))
        return back(k_out), back(v_out), cand

    return jax.shard_map(local_step, mesh=mesh, in_specs=in_specs, out_specs=out_specs, check_vma=False)
```
